128 devices in a mesh: batch: 1, outer: 2 (over core), rows: 64 (over z, y, x).
Axes of the slice: x: 4, y: 4, z: 4, core: 2. Of those that a mesh axis runs over, the one named last changes fastest.
Arguments:
- a_mat: float32 [131072, 768], P(('batch', 'outer', 'rows'))
Outputs:
- output 1: float32 [131072, 768], P(('batch', 'outer', 'rows'))
- output 2: float32 [768, 768], P('batch')
All inputs are finite; a program needn't handle non-finite values.
Results may differ from the reference program's by a relative error of at most 0.001.
Values sent between devices are 32-bit elements.
A program may use at most 1 GiB of HBM per device.

```python
import jax
import jax.numpy as jnp
from jax import lax

TOTAL_ROWS = 131072
N_COLS = 768


def gram_of(row_blk):
    return lax.dot_general(row_blk, row_blk, (((0,), (0,)), ((), ())), precision=lax.Precision.HIGHEST, preferred_element_type=jnp.float32)


def chol_sweep(row_blk):
    low_fac = jnp.linalg.cholesky(gram_of(row_blk))
    solved = lax.linalg.triangular_solve(low_fac, row_blk, left_side=False, lower=True, transpose_a=True)
    return solved, low_fac


def setup_inputs(seed: int = 0, part: int = 0) -> dict:
    key = jax.random.fold_in(jax.random.key(seed), part)
    key_rows, key_mix = jax.random.split(key)
    base_rows = jax.random.normal(key_rows, (TOTAL_ROWS, N_COLS), jnp.float32)
    ortho_mix = jnp.linalg.qr(jax.random.normal(key_mix, (N_COLS, N_COLS), jnp.float32))[0]
    col_idx = jnp.arange(N_COLS, dtype=jnp.float32)
    spectrum = jnp.power(10.0, -3.0 * col_idx / (N_COLS - 1))
    mixing = spectrum[:, None] * ortho_mix.T
    a_mat = jnp.dot(base_rows, mixing, precision=lax.Precision.HIGHEST, preferred_element_type=jnp.float32)
    return {"a_mat": a_mat}


def reference(a_mat):
    q_one, low_one = chol_sweep(a_mat)
    q_two, low_two = chol_sweep(q_one)
    r_fac = lax.dot_general(low_two, low_one, (((0,), (1,)), ((), ())), precision=lax.Precision.HIGHEST, preferred_element_type=jnp.float32)
    return q_two, r_fac
```

```python
import functools
import jax, jax.numpy as jnp
from jax import lax
from jax.experimental import pallas as pl
from jax.experimental.pallas import tpu as pltpu
from jax.sharding import PartitionSpec as P
MESH = pl.DeviceIdType.MESH
ROWS = 3072
HALF = 1536
NCH = 64
CH = 24

def ids():
    return lax.axis_index("outer"), lax.axis_index("rows")

def ar_direct(p_ref, o_ref, recv0, acc, recv1, red, s0, r0, s1, r1, s2, r2, s3, r3):
    c, me = ids()
    other = 1 - c
    bar = pltpu.get_barrier_semaphore()
    pl.semaphore_signal(bar, inc=1, device_id=(0, other, me), device_id_type=MESH)
    def sig(k, _):
        pl.semaphore_signal(bar, inc=1, device_id=(0, c, lax.rem(me + k, NCH)), device_id_type=MESH)
        return 0
    lax.fori_loop(1, NCH, sig, 0)
    pl.semaphore_wait(bar, NCH)
    cp = pltpu.make_async_remote_copy(p_ref.at[pl.ds(pl.multiple_of(other * HALF, 8), HALF)], recv0, s0, r0, device_id=(0, other, me), device_id_type=MESH)
    cp.start()
    cp.wait()
    acc[...] = p_ref[pl.ds(pl.multiple_of(c * HALF, 8), HALF)] + recv0[...]
    def mk1(k):
        peer = lax.rem(me + k, NCH)
        return pltpu.make_async_remote_copy(acc.at[pl.ds(pl.multiple_of(peer * CH, 8), CH)], recv1.at[pl.ds(pl.multiple_of((k - 1) * CH, 8), CH)], s1, r1, device_id=(0, c, peer), device_id_type=MESH)
    def st1(k, _):
        mk1(k).start()
        return 0
    lax.fori_loop(1, NCH, st1, 0)
    big = pltpu.make_async_remote_copy(acc.at[pl.ds(0, 63 * CH)], recv1, s1, r1, device_id=(0, c, me), device_id_type=MESH)
    big.wait_recv()
    tot = acc[pl.ds(pl.multiple_of(me * CH, 8), CH)]
    tot = lax.fori_loop(0, 63, lambda k, t: t + recv1[pl.ds(pl.multiple_of(k * CH, 8), CH)], tot)
    red[...] = tot
    off = pl.multiple_of(c * HALF + me * CH, 8)
    def st2(k, _):
        peer = lax.rem(me + k, NCH)
        pltpu.make_async_remote_copy(red, o_ref.at[pl.ds(off, CH)], s2, r2, device_id=(0, c, peer), device_id_type=MESH).start()
        return 0
    lax.fori_loop(1, NCH, st2, 0)
    o_ref[pl.ds(off, CH)] = tot
    big2 = pltpu.make_async_remote_copy(acc.at[pl.ds(0, 63 * CH)], recv1, s2, r2, device_id=(0, c, me), device_id_type=MESH)
    big2.wait_recv()
    half = pl.ds(pl.multiple_of(c * HALF, 8), HALF)
    cp3 = pltpu.make_async_remote_copy(o_ref.at[half], o_ref.at[half], s3, r3, device_id=(0, other, me), device_id_type=MESH)
    cp3.start()
    cp3.wait()
    big.wait_send()
    big2.wait_send()

def call_direct(p):
    return pl.pallas_call(
        ar_direct, out_shape=jax.ShapeDtypeStruct((ROWS, 128), jnp.float32),
        in_specs=[pl.BlockSpec(memory_space=pltpu.VMEM)], out_specs=pl.BlockSpec(memory_space=pltpu.VMEM),
        scratch_shapes=[pltpu.VMEM((HALF, 128), jnp.float32), pltpu.VMEM((HALF, 128), jnp.float32), pltpu.VMEM((63 * CH, 128), jnp.float32), pltpu.VMEM((CH, 128), jnp.float32)] + [pltpu.SemaphoreType.DMA] * 8,
        compiler_params=pltpu.CompilerParams(collective_id=0, has_side_effects=True), name="ar_direct")(p)


PAIRS = ((0, 0), (0, 1), (0, 2), (1, 1), (1, 2), (2, 2))
HI = lax.Precision.HIGHEST


def gram(x):
    blks = []
    for i, j in PAIRS:
        b = lax.dot_general(x[:, 256 * i:256 * i + 256], x[:, 256 * j:256 * j + 256], (((0,), (0,)), ((), ())), precision=HI, preferred_element_type=jnp.float32)
        blks += [b[:, :128], b[:, 128:]]
    s = call_direct(jnp.concatenate(blks, axis=0))
    full = {}
    for n, (i, j) in enumerate(PAIRS):
        b = jnp.concatenate([s[512 * n:512 * n + 256], s[512 * n + 256:512 * n + 512]], axis=1)
        full[i, j] = b
        if i != j:
            full[j, i] = b.T
    return jnp.concatenate([jnp.concatenate([full[i, j] for j in range(3)], axis=1) for i in range(3)], axis=0)


def sweep(x):
    low = jnp.linalg.cholesky(gram(x))
    return lax.linalg.triangular_solve(low, x, left_side=False, lower=True, transpose_a=True), low


def solution(mesh):
    spec = P(("batch", "outer", "rows"), None)

    def local_qr(a):
        q1, l1 = sweep(a)
        q2, l2 = sweep(q1)
        r = lax.dot_general(l2, l1, (((0,), (1,)), ((), ())), precision=HI, preferred_element_type=jnp.float32)
        return q2, r

    return jax.shard_map(local_qr, mesh=mesh, in_specs=(spec,), out_specs=(spec, P("batch", None)), check_vma=False)
```

```python
import functools
import jax, jax.numpy as jnp
from jax import lax
from jax.experimental import pallas as pl
from jax.experimental.pallas import tpu as pltpu
from jax.sharding import PartitionSpec as P
MESH = pl.DeviceIdType.MESH
ROWS = 3072
HALF = 1536
NCH = 64
CH = 24

def ids():
    return lax.axis_index("outer"), lax.axis_index("rows")

def ar_direct(p_ref, o_ref, recv0, acc, recv1, red, s0, r0, s1, r1, s2, r2, s3, r3):
    c, me = ids()
    other = 1 - c
    bar = pltpu.get_barrier_semaphore()
    pl.semaphore_signal(bar, inc=1, device_id=(0, other, me), device_id_type=MESH)
    def sig(k, _):
        pl.semaphore_signal(bar, inc=1, device_id=(0, c, lax.rem(me + k, NCH)), device_id_type=MESH)
        return 0
    lax.fori_loop(1, NCH, sig, 0)
    pl.semaphore_wait(bar, NCH)
    cp = pltpu.make_async_remote_copy(p_ref.at[pl.ds(pl.multiple_of(other * HALF, 8), HALF)], recv0, s0, r0, device_id=(0, other, me), device_id_type=MESH)
    cp.start()
    cp.wait()
    acc[...] = p_ref[pl.ds(pl.multiple_of(c * HALF, 8), HALF)] + recv0[...]
    def mk1(k):
        peer = lax.rem(me + k, NCH)
        return pltpu.make_async_remote_copy(acc.at[pl.ds(pl.multiple_of(peer * CH, 8), CH)], recv1.at[pl.ds(pl.multiple_of((k - 1) * CH, 8), CH)], s1, r1, device_id=(0, c, peer), device_id_type=MESH)
    def st1(k, _):
        mk1(k).start()
        return 0
    lax.fori_loop(1, NCH, st1, 0)
    big = pltpu.make_async_remote_copy(acc.at[pl.ds(0, 63 * CH)], recv1, s1, r1, device_id=(0, c, me), device_id_type=MESH)
    big.wait_recv()
    tot = acc[pl.ds(pl.multiple_of(me * CH, 8), CH)]
    tot = lax.fori_loop(0, 63, lambda k, t: t + recv1[pl.ds(pl.multiple_of(k * CH, 8), CH)], tot)
    red[...] = tot
    off = pl.multiple_of(c * HALF + me * CH, 8)
    def st2(k, _):
        peer = lax.rem(me + k, NCH)
        pltpu.make_async_remote_copy(red, o_ref.at[pl.ds(off, CH)], s2, r2, device_id=(0, c, peer), device_id_type=MESH).start()
        return 0
    lax.fori_loop(1, NCH, st2, 0)
    o_ref[pl.ds(off, CH)] = tot
    big2 = pltpu.make_async_remote_copy(acc.at[pl.ds(0, 63 * CH)], recv1, s2, r2, device_id=(0, c, me), device_id_type=MESH)
    big2.wait_recv()
    half = pl.ds(pl.multiple_of(c * HALF, 8), HALF)
    cp3 = pltpu.make_async_remote_copy(o_ref.at[half], o_ref.at[half], s3, r3, device_id=(0, other, me), device_id_type=MESH)
    cp3.start()
    cp3.wait()
    big.wait_send()
    big2.wait_send()

def call_direct(p):
    return pl.pallas_call(
        ar_direct, out_shape=jax.ShapeDtypeStruct((ROWS, 128), jnp.float32),
        in_specs=[pl.BlockSpec(memory_space=pltpu.VMEM)], out_specs=pl.BlockSpec(memory_space=pltpu.VMEM),
        scratch_shapes=[pltpu.VMEM((HALF, 128), jnp.float32), pltpu.VMEM((HALF, 128), jnp.float32), pltpu.VMEM((63 * CH, 128), jnp.float32), pltpu.VMEM((CH, 128), jnp.float32)] + [pltpu.SemaphoreType.DMA] * 8,
        compiler_params=pltpu.CompilerParams(collective_id=0, has_side_effects=True), name="ar_direct")(p)


HI = lax.Precision.HIGHEST
PAIRS = ((0, 0), (0, 1), (0, 2), (1, 1), (1, 2), (2, 2))
N = 768
NB = 6

def dot(a, b, dims):
    return lax.dot_general(a, b, (dims, ((), ())), precision=HI, preferred_element_type=jnp.float32)

def bl(x, l):
    return jnp.broadcast_to(x[:, l:l + 1], (8, 128))

def bs(x, s):
    return jnp.broadcast_to(x[s:s + 1, :], (8, 128))

def factor(dref, uref, mref):
    sub = lax.broadcasted_iota(jnp.int32, (8, 128), 0)
    lane = lax.broadcasted_iota(jnp.int32, (8, 128), 1)
    zero = jnp.zeros((8, 128), jnp.float32)
    A = [dref[8 * i:8 * i + 8, :] for i in range(16)]
    B = [jnp.where(lane == sub + 8 * i, 1.0, zero) for i in range(16)]
    for p in range(16):
        c = [bl(A[p], 8 * p + s) for s in range(8)]
        P, Q = A[p], B[p]
        rinv, ls, lb, ur, vr = [], [], {}, [], []
        for s in range(8):
            ri = lax.rsqrt(bs(c[s], s))
            l = c[s] * ri
            for t in range(s + 1, 8):
                b = bs(l, t)
                lb[s, t] = b
                c[t] = c[t] - l * b
            m = jnp.where(sub > s, l, 0.0)
            u = bs(P, s) * ri
            v = bs(Q, s) * ri
            P = jnp.where(sub == s, u, P - m * u)
            Q = jnp.where(sub == s, v, Q - m * v)
            rinv.append(ri); ur.append(u); vr.append(v)
        uref[8 * p:8 * p + 8, :] = jnp.where(lane >= sub + 8 * p, P, 0.0)
        mref[8 * p:8 * p + 8, :] = Q
        for i in range(p + 1, 16):
            d = [bl(A[i], 8 * p + s) for s in range(8)]
            a, b_ = A[i], B[i]
            for s in range(8):
                l = d[s] * rinv[s]
                for t in range(s + 1, 8):
                    d[t] = d[t] - l * lb[s, t]
                a = a - l * ur[s]
                b_ = b_ - l * vr[s]
            A[i], B[i] = a, b_


def unpack(s_ref, g):
    for n, (i, j) in enumerate(PAIRS):
        for h in range(2):
            g[256 * i:256 * i + 256, 256 * j + 128 * h:256 * j + 128 * h + 128] = s_ref[512 * n + 256 * h:512 * n + 256 * h + 256, :]


def gram_pack(x_ref, p_ref):
    for n, (i, j) in enumerate(PAIRS):
        b = dot(x_ref[:, 256 * i:256 * i + 256], x_ref[:, 256 * j:256 * j + 256], ((0,), (0,)))
        p_ref[512 * n:512 * n + 256, :] = b[:, :128]
        p_ref[512 * n + 256:512 * n + 512, :] = b[:, 128:]


def chol_inv(g, u_ref, m_ref, dbuf, ubuf, mbuf):
    def step(k, _):
        for kk in range(NB):
            @pl.when(k == kk)
            def _():
                dbuf[...] = g[128 * kk:128 * kk + 128, 128 * kk:128 * kk + 128]
        factor(dbuf, ubuf, mbuf)
        for kk in range(NB):
            @pl.when(k == kk)
            def _():
                lo, hi = 128 * kk, 128 * kk + 128
                w = mbuf[...]
                u_ref[lo:hi, lo:hi] = ubuf[...]
                if kk > 0:
                    m_ref[lo:hi, :lo] = dot(w, m_ref[lo:hi, :lo], ((1,), (0,)))
                m_ref[lo:hi, lo:hi] = w
                if kk < NB - 1:
                    u_ref[lo:hi, hi:] = dot(w, g[lo:hi, hi:], ((1,), (0,)))
                    for i in range(kk + 1, NB):
                        a, b = 128 * i, 128 * i + 128
                        ut = u_ref[lo:hi, a:b]
                        g[a:b, a:] = g[a:b, a:] - dot(ut, u_ref[lo:hi, a:], ((0,), (0,)))
                        m_ref[a:b, :hi] = m_ref[a:b, :hi] - dot(ut, m_ref[lo:hi, :hi], ((0,), (0,)))
        return 0

    lax.fori_loop(0, NB, step, 0)


def apply_inv(x_ref, m_ref, q_ref):
    def rows(r, _):
        sl = pl.ds(pl.multiple_of(256 * r, 256), 256)
        for j in range(3):
            q_ref[sl, 256 * j:256 * j + 256] = dot(x_ref[sl, :256 * j + 256], m_ref[256 * j:256 * j + 256, :256 * j + 256], ((1,), (1,)))
        return 0
    lax.fori_loop(0, x_ref.shape[0] // 256, rows, 0)


def gram_kernel(x_ref, p_ref):
    gram_pack(x_ref, p_ref)


def first_kernel(s_ref, x_ref, q_ref, u_ref, p_ref, g, m, dbuf, ubuf, mbuf):
    unpack(s_ref, g)
    u_ref[...] = jnp.zeros_like(u_ref)
    m[...] = jnp.zeros_like(m)
    chol_inv(g, u_ref, m, dbuf, ubuf, mbuf)
    apply_inv(x_ref, m, q_ref)
    gram_pack(q_ref, p_ref)


def second_kernel(s_ref, x_ref, u1_ref, q_ref, r_ref, g, u, m, dbuf, ubuf, mbuf):
    unpack(s_ref, g)
    u[...] = jnp.zeros_like(u)
    m[...] = jnp.zeros_like(m)
    chol_inv(g, u, m, dbuf, ubuf, mbuf)
    apply_inv(x_ref, m, q_ref)
    for i in range(3):
        for j in range(3):
            a, b = slice(256 * i, 256 * i + 256), slice(256 * j, 256 * j + 256)
            if i > j:
                r_ref[a, b] = jnp.zeros((256, 256), jnp.float32)
            else:
                k = slice(256 * i, 256 * j + 256)
                r_ref[a, b] = dot(u[a, k], u1_ref[k, b], ((1,), (0,)))


def vcall(kern, name, outs, scratch, *args):
    V = pl.BlockSpec(memory_space=pltpu.VMEM)
    return pl.pallas_call(
        kern, out_shape=tuple(jax.ShapeDtypeStruct(o, jnp.float32) for o in outs),
        in_specs=[V] * len(args), out_specs=(V,) * len(outs),
        scratch_shapes=[pltpu.VMEM(s, jnp.float32) for s in scratch],
        compiler_params=pltpu.CompilerParams(vmem_limit_bytes=50 * 2**20), name=name)(*args)


NN = (N, N)
SMALL = [(128, 128)] * 3


def solution(mesh):
    spec = P(("batch", "outer", "rows"), None)

    def local_qr(a):
        p1, = vcall(gram_kernel, "gram", [(ROWS, 128)], [], a)
        s1 = call_direct(p1)
        q1, u1, p2 = vcall(first_kernel, "first", [a.shape, NN, (ROWS, 128)], [NN, NN] + SMALL, s1, a)
        s2 = call_direct(p2)
        q2, r = vcall(second_kernel, "second", [a.shape, NN], [NN, NN, NN] + SMALL, s2, q1, u1)
        return q2, r

    return jax.shard_map(local_qr, mesh=mesh, in_specs=(spec,), out_specs=(spec, P("batch", None)), check_vma=False)
```

```python
import functools
import jax
import jax.numpy as jnp
from jax import lax
from jax.experimental import pallas as pl
from jax.experimental.pallas import tpu as pltpu
from jax.sharding import PartitionSpec as P

MESH = pl.DeviceIdType.MESH
HI = lax.Precision.HIGHEST
N = 768
NB = 6
ROWS = 3072
HALF = 1536
NCH = 64
CH = 24
PAIRS = ((0, 0), (0, 1), (0, 2), (1, 1), (1, 2), (2, 2))


def dot(a, b, dims):
    return lax.dot_general(a, b, (dims, ((), ())), precision=HI, preferred_element_type=jnp.float32)


def m8(v):
    return pl.multiple_of(v, 8)


def unpack(s_ref, g):
    for n, (i, j) in enumerate(PAIRS):
        for h in range(2):
            g[256 * i:256 * i + 256, 256 * j + 128 * h:256 * j + 128 * h + 128] = s_ref[512 * n + 256 * h:512 * n + 256 * h + 256, :]


def bl(x, l):
    return jnp.broadcast_to(x[:, l:l + 1], (8, 128))

def bs(x, s):
    return jnp.broadcast_to(x[s:s + 1, :], (8, 128))

def factor(dref, uref, mref):
    sub = lax.broadcasted_iota(jnp.int32, (8, 128), 0)
    lane = lax.broadcasted_iota(jnp.int32, (8, 128), 1)
    zero = jnp.zeros((8, 128), jnp.float32)
    A = [dref[8 * i:8 * i + 8, :] for i in range(16)]
    for sp in range(8):
        l0 = 16 * sp
        ia, ib = 2 * sp, 2 * sp + 1
        blk = (lane >= l0) & (lane < l0 + 16)
        Ua, Ub = A[ia], A[ib]
        ca = [bl(Ua, l0 + s) for s in range(8)]
        cb = [bl(Ub, l0 + s) for s in range(16)]
        urg = [n for n in (ia + 2, ia + 3) if n < 16]
        cn = {n: [bl(A[n], l0 + s) for s in range(16)] for n in urg}
        Wa = jnp.where(blk, jnp.where(lane == sub + l0, 1.0, zero), Ua)
        Wb = jnp.where(blk, jnp.where(lane == sub + (l0 + 8), 1.0, zero), Ub)
        for n in range(ia + 2, 16):
            A[n] = jnp.where(blk, zero, A[n])
        for s in range(16):
            first = s < 8
            r = s % 8
            ri = lax.rsqrt(bs(ca[s] if first else cb[s], r))
            lb = cb[s] * ri
            if first:
                la = ca[s] * ri
                L = {t: (bs(la, t) if t < 8 else bs(lb, t - 8)) for t in range(s + 1, 16)}
                for t in range(s + 1, 8):
                    ca[t] = ca[t] - la * L[t]
                ma = jnp.where(sub > r, la, zero)
                u, w = bs(Ua, r) * ri, bs(Wa, r) * ri
                Ua = jnp.where(sub == r, u, Ua - ma * u)
                Wa = jnp.where(sub == r, w, Wa - ma * w)
                Ub = Ub - lb * u
                Wb = Wb - lb * w
            else:
                L = {t: bs(lb, t - 8) for t in range(s + 1, 16)}
                mb = jnp.where(sub > r, lb, zero)
                u, w = bs(Ub, r) * ri, bs(Wb, r) * ri
                Ub = jnp.where(sub == r, u, Ub - mb * u)
                Wb = jnp.where(sub == r, w, Wb - mb * w)
            for t in range(s + 1, 16):
                cb[t] = cb[t] - lb * L[t]
            for n in urg:
                ln = cn[n][s] * ri
                for t in range(s + 1, 16):
                    cn[n][t] = cn[n][t] - ln * L[t]
                A[n] = A[n] - ln * w
        uref[l0:l0 + 8, :] = jnp.where(lane >= sub + l0, Ua, zero)
        uref[l0 + 8:l0 + 16, :] = jnp.where(lane >= sub + (l0 + 8), Ub, zero)
        keep = lane < l0 + 16
        mref[l0:l0 + 8, :] = jnp.where(keep, Wa, zero)
        mref[l0 + 8:l0 + 16, :] = jnp.where(keep, Wb, zero)
        if ia + 4 < 16:
            W = jnp.concatenate([Wa, Wb], axis=0)
            D = dot(W, W, ((0,), (0,)))
            for n in range(ia + 4, 16):
                A[n] = A[n] - D[8 * n:8 * n + 8, :]


def chol_inv(g, u_ref, m_ref, dbuf, ubuf, mbuf):
    def step(k, _):
        for kk in range(NB):
            @pl.when(k == kk)
            def _():
                dbuf[...] = g[128 * kk:128 * kk + 128, 128 * kk:128 * kk + 128]
        factor(dbuf, ubuf, mbuf)
        for kk in range(NB):
            @pl.when(k == kk)
            def _():
                lo, hi = 128 * kk, 128 * kk + 128
                w = mbuf[...]
                u_ref[lo:hi, lo:hi] = ubuf[...]
                if kk > 0:
                    m_ref[lo:hi, :lo] = dot(w, m_ref[lo:hi, :lo], ((1,), (0,)))
                m_ref[lo:hi, lo:hi] = w
                if kk < NB - 1:
                    u_ref[lo:hi, hi:] = dot(w, g[lo:hi, hi:], ((1,), (0,)))
                    for i in range(kk + 1, NB):
                        a, b = 128 * i, 128 * i + 128
                        ut = u_ref[lo:hi, a:b]
                        g[a:b, a:] = g[a:b, a:] - dot(ut, u_ref[lo:hi, a:], ((0,), (0,)))
                        m_ref[a:b, :hi] = m_ref[a:b, :hi] - dot(ut, m_ref[lo:hi, :hi], ((0,), (0,)))
        return 0

    lax.fori_loop(0, NB, step, 0)


def apply_inv(x_ref, m_ref, q_ref):
    def rows(r, _):
        sl = pl.ds(pl.multiple_of(256 * r, 256), 256)
        for j in range(3):
            q_ref[sl, 256 * j:256 * j + 256] = dot(x_ref[sl, :256 * j + 256], m_ref[256 * j:256 * j + 256, :256 * j + 256], ((1,), (1,)))
        return 0
    lax.fori_loop(0, x_ref.shape[0] // 256, rows, 0)


def greet(c, me):
    bar = pltpu.get_barrier_semaphore()
    pl.semaphore_signal(bar, inc=1, device_id=(0, 1 - c, me), device_id_type=MESH)

    def sig(k, _):
        pl.semaphore_signal(bar, inc=1, device_id=(0, c, lax.rem(me + k, NCH)), device_id_type=MESH)
        return 0
    lax.fori_loop(1, NCH, sig, 0)
    return bar


def gram_half(x_ref, p_ref, half):
    def blk(t, _):
        n = 3 * half + t
        i = n // 3 + n // 5
        j = n - 2 * (n // 3) - n // 5
        b = dot(x_ref[:, pl.ds(pl.multiple_of(256 * i, 256), 256)], x_ref[:, pl.ds(pl.multiple_of(256 * j, 256), 256)], ((0,), (0,)))
        p_ref[pl.ds(m8(512 * n), 256), :] = b[:, :128]
        p_ref[pl.ds(m8(512 * n + 256), 256), :] = b[:, 128:]
        return 0
    lax.fori_loop(0, 3, blk, 0)


def gram_sum(bar, c, me, x_ref, p, o, recv0, acc, recv1, red, s0, r0, s1, r1, s2, r2, s3, r3):
    other = 1 - c
    gram_half(x_ref, p, other)
    pl.semaphore_wait(bar, NCH)
    mine = pl.ds(m8(c * HALF), HALF)
    cp = pltpu.make_async_remote_copy(p.at[pl.ds(m8(other * HALF), HALF)], recv0, s0, r0, device_id=(0, other, me), device_id_type=MESH)
    cp.start()
    gram_half(x_ref, p, c)
    cp.wait()
    acc[...] = p[mine] + recv0[...]

    def st1(k, _):
        peer = lax.rem(me + k, NCH)
        pltpu.make_async_remote_copy(acc.at[pl.ds(m8(peer * CH), CH)], recv1.at[pl.ds(m8((k - 1) * CH), CH)], s1, r1, device_id=(0, c, peer), device_id_type=MESH).start()
        return 0
    lax.fori_loop(1, NCH, st1, 0)
    big = pltpu.make_async_remote_copy(acc.at[pl.ds(0, 63 * CH)], recv1, s1, r1, device_id=(0, c, me), device_id_type=MESH)
    big.wait_recv()
    tot = lax.fori_loop(0, 63, lambda k, t: t + recv1[pl.ds(m8(k * CH), CH)], acc[pl.ds(m8(me * CH), CH)])
    red[...] = tot
    off = m8(c * HALF + me * CH)

    def st2(k, _):
        peer = lax.rem(me + k, NCH)
        pltpu.make_async_remote_copy(red, o.at[pl.ds(off, CH)], s2, r2, device_id=(0, c, peer), device_id_type=MESH).start()
        return 0
    lax.fori_loop(1, NCH, st2, 0)
    o[pl.ds(off, CH)] = tot
    big2 = pltpu.make_async_remote_copy(acc.at[pl.ds(0, 63 * CH)], recv1, s2, r2, device_id=(0, c, me), device_id_type=MESH)
    big2.wait_recv()
    cp3 = pltpu.make_async_remote_copy(o.at[mine], o.at[mine], s3, r3, device_id=(0, other, me), device_id_type=MESH)
    cp3.start()
    cp3.wait()
    big.wait_send()
    big2.wait_send()


def apply_inv(x_ref, m_ref, q_ref):
    def rows(r, _):
        sl = pl.ds(pl.multiple_of(256 * r, 256), 256)
        for j in range(3):
            q_ref[sl, 256 * j:256 * j + 256] = dot(x_ref[sl, :256 * j + 256], m_ref[256 * j:256 * j + 256, :256 * j + 256], ((1,), (1,)))
        return 0
    lax.fori_loop(0, x_ref.shape[0] // 256, rows, 0)


def clear(*refs):
    for r in refs:
        r[...] = jnp.zeros_like(r)


def first_kernel(x_ref, m_ref, u_ref, g, dbuf, ubuf, mbuf, *comm):
    c, me = lax.axis_index("outer"), lax.axis_index("rows")
    bar = greet(c, me)
    clear(m_ref, u_ref)
    gram_sum(bar, c, me, x_ref, *comm)
    unpack(comm[1], g)
    chol_inv(g, u_ref, m_ref, dbuf, ubuf, mbuf)


def second_kernel(x_ref, m1_ref, q_ref, m_ref, u_ref, g, dbuf, ubuf, mbuf, *comm):
    c, me = lax.axis_index("outer"), lax.axis_index("rows")
    bar = greet(c, me)
    clear(m_ref, u_ref)
    apply_inv(x_ref, m1_ref, q_ref)
    gram_sum(bar, c, me, q_ref, *comm)
    unpack(comm[1], g)
    chol_inv(g, u_ref, m_ref, dbuf, ubuf, mbuf)


def third_kernel(x_ref, m_ref, u2_ref, u1_ref, q_ref, r_ref):
    apply_inv(x_ref, m_ref, q_ref)
    for i in range(3):
        for j in range(3):
            a, b = slice(256 * i, 256 * i + 256), slice(256 * j, 256 * j + 256)
            if i > j:
                r_ref[a, b] = jnp.zeros((256, 256), jnp.float32)
            else:
                k = slice(256 * i, 256 * j + 256)
                r_ref[a, b] = dot(u2_ref[a, k], u1_ref[k, b], ((1,), (0,)))


NN = (N, N)
BUFS = [NN, (128, 128), (128, 128), (128, 128), (ROWS, 128), (ROWS, 128), (HALF, 128), (HALF, 128), (63 * CH, 128), (CH, 128)]


def vcall(kern, name, outs, args, cid=None):
    V = pl.BlockSpec(memory_space=pltpu.VMEM)
    scratch = [] if cid is None else [pltpu.VMEM(s, jnp.float32) for s in BUFS] + [pltpu.SemaphoreType.DMA] * 8
    params = {} if cid is None else dict(collective_id=cid, has_side_effects=True)
    return pl.pallas_call(
        kern, out_shape=tuple(jax.ShapeDtypeStruct(o, jnp.float32) for o in outs),
        in_specs=[V] * len(args), out_specs=(V,) * len(outs), scratch_shapes=scratch,
        compiler_params=pltpu.CompilerParams(vmem_limit_bytes=50 * 2**20, **params), name=name)(*args)


def solution(mesh):
    spec = P(("batch", "outer", "rows"), None)

    def local_qr(a):
        m1, u1 = vcall(first_kernel, "first", [NN, NN], [a], 0)
        q1, m2, u2 = vcall(second_kernel, "second", [a.shape, NN, NN], [a, m1], 1)
        return tuple(vcall(third_kernel, "third", [a.shape, NN], [q1, m2, u2, u1]))

    return jax.shard_map(local_qr, mesh=mesh, in_specs=(spec,), out_specs=(spec, P("batch", None)), check_vma=False)
```

```python
import jax
import jax.numpy as jnp
from jax import lax
from jax.experimental import pallas as pl
from jax.experimental.pallas import tpu as pltpu
from jax.sharding import PartitionSpec as P

MESH = pl.DeviceIdType.MESH
HI = lax.Precision.HIGHEST
NT = ((1,), (1,))
N = 768
NB = 6
NCH = 64
CHUNKS = ((0, 2, 0), (2, 4, 24), (4, 5, 16), (5, 6, 56))
BLKS = tuple(tuple((i, j) for i in range(a, b) for j in range(i + 1)) for a, b, _ in CHUNKS)
UNITS = tuple(8 * len(b) for b in BLKS)


def dot(a, b, dims):
    return lax.dot_general(a, b, (dims, ((), ())), precision=HI, preferred_element_type=jnp.float32)


def m8(v):
    return pl.multiple_of(v, 8)


def rb(i, j=None):
    return slice(128 * i, 128 * (i + 1 if j is None else j))


def bl(x, l):
    return jnp.broadcast_to(x[:, l:l + 1], (8, 128))

def bs(x, s):
    return jnp.broadcast_to(x[s:s + 1, :], (8, 128))

def factor(dref, uref, mref):
    sub = lax.broadcasted_iota(jnp.int32, (8, 128), 0)
    lane = lax.broadcasted_iota(jnp.int32, (8, 128), 1)
    zero = jnp.zeros((8, 128), jnp.float32)
    A = [dref[8 * i:8 * i + 8, :] for i in range(16)]
    for sp in range(8):
        l0 = 16 * sp
        ia, ib = 2 * sp, 2 * sp + 1
        blk = (lane >= l0) & (lane < l0 + 16)
        Ua, Ub = A[ia], A[ib]
        ca = [bl(Ua, l0 + s) for s in range(8)]
        cb = [bl(Ub, l0 + s) for s in range(16)]
        urg = [n for n in (ia + 2, ia + 3) if n < 16]
        cn = {n: [bl(A[n], l0 + s) for s in range(16)] for n in urg}
        Wa = jnp.where(blk, jnp.where(lane == sub + l0, 1.0, zero), Ua)
        Wb = jnp.where(blk, jnp.where(lane == sub + (l0 + 8), 1.0, zero), Ub)
        for n in range(ia + 2, 16):
            A[n] = jnp.where(blk, zero, A[n])
        for s in range(16):
            first = s < 8
            r = s % 8
            ri = lax.rsqrt(bs(ca[s] if first else cb[s], r))
            lb = cb[s] * ri
            if first:
                la = ca[s] * ri
                L = {t: (bs(la, t) if t < 8 else bs(lb, t - 8)) for t in range(s + 1, 16)}
                for t in range(s + 1, 8):
                    ca[t] = ca[t] - la * L[t]
                ma = jnp.where(sub > r, la, zero)
                u, w = bs(Ua, r) * ri, bs(Wa, r) * ri
                Ua = jnp.where(sub == r, u, Ua - ma * u)
                Wa = jnp.where(sub == r, w, Wa - ma * w)
                Ub = Ub - lb * u
                Wb = Wb - lb * w
            else:
                L = {t: bs(lb, t - 8) for t in range(s + 1, 16)}
                mb = jnp.where(sub > r, lb, zero)
                u, w = bs(Ub, r) * ri, bs(Wb, r) * ri
                Ub = jnp.where(sub == r, u, Ub - mb * u)
                Wb = jnp.where(sub == r, w, Wb - mb * w)
            for t in range(s + 1, 16):
                cb[t] = cb[t] - lb * L[t]
            for n in urg:
                ln = cn[n][s] * ri
                for t in range(s + 1, 16):
                    cn[n][t] = cn[n][t] - ln * L[t]
                A[n] = A[n] - ln * w
        uref[l0:l0 + 8, :] = jnp.where(lane >= sub + l0, Ua, zero)
        uref[l0 + 8:l0 + 16, :] = jnp.where(lane >= sub + (l0 + 8), Ub, zero)
        keep = lane < l0 + 16
        mref[l0:l0 + 8, :] = jnp.where(keep, Wa, zero)
        mref[l0 + 8:l0 + 16, :] = jnp.where(keep, Wb, zero)
        if ia + 4 < 16:
            W = jnp.concatenate([Wa, Wb], axis=0)
            D = dot(W, W, ((0,), (0,)))
            for n in range(ia + 4, 16):
                A[n] = A[n] - D[8 * n:8 * n + 8, :]


class Sum:
    def __init__(self, ch, c, me, bufs, sems):
        self.ch, self.c, self.me, self.other = ch, c, me, 1 - c
        self.p, self.recv0, self.acc, self.recv1, self.o, self.red = bufs
        self.s0, self.r0, self.s1, self.r1, self.s2, self.r2, self.s3, self.r3 = sems
        self.U = UNITS[ch]
        self.half = 8 * self.U
        self.base = CHUNKS[ch][2]
        self.mine = pl.ds(m8(c * self.half), self.half)
        self.unit = lax.rem(me - self.base + NCH, NCH)

    def gram(self, x):
        a, b, _ = CHUNKS[self.ch]
        full = dot(x[:, rb(a, b)], x[:, rb(0, b)], ((0,), (0,)))
        for n, (i, j) in enumerate(BLKS[self.ch]):
            self.p[rb(n), :] = full[rb(i - a), rb(j)]

    def exch(self, ref, dst, s, r, sl):
        return pltpu.make_async_remote_copy(ref.at[sl], dst, s, r, device_id=(0, self.other, self.me), device_id_type=MESH)

    def swap(self):
        sl = pl.ds(m8(self.other * self.half), self.half)
        self.cp0 = self.exch(self.p, self.recv0, self.s0, self.r0, sl)
        self.cp0.start()

    def scatter(self):
        self.exch(self.p, self.recv0, self.s0, self.r0, self.mine).wait_recv()
        self.acc[...] = self.p[self.mine] + self.recv0[...]

        def send(i, _):
            u = lax.rem(self.me + i, self.U)
            peer = lax.rem(self.base + u, NCH)
            k = lax.rem(peer - self.me + NCH, NCH)

            @pl.when(k > 0)
            def _():
                pltpu.make_async_remote_copy(self.acc.at[pl.ds(m8(8 * u), 8)], self.recv1.at[pl.ds(m8(8 * k - 8), 8)], self.s1, self.r1, device_id=(0, self.c, peer), device_id_type=MESH).start()
            return 0
        lax.fori_loop(0, self.U, send, 0)

    def rows(self, n, s, r):
        return pltpu.make_async_remote_copy(self.recv1.at[pl.ds(0, 8 * n)], self.recv1.at[pl.ds(0, 8 * n)], s, r, device_id=(0, self.other, self.me), device_id_type=MESH)

    def reduce(self):
        @pl.when(self.unit < self.U)
        def _():
            self.rows(63, self.s1, self.r1).wait_recv()
            t = [self.acc[pl.ds(m8(8 * self.unit), 8)]] + [self.recv1[8 * k:8 * k + 8, :] for k in range(63)]
            while len(t) > 1:
                t = [t[i] + t[i + 1] for i in range(0, len(t), 2)]
            self.red[...] = t[0]
            dst = pl.ds(m8(self.c * self.half + 8 * self.unit), 8)

            def send(k, _):
                peer = lax.rem(self.me + k, NCH)
                pltpu.make_async_remote_copy(self.red, self.o.at[dst], self.s2, self.r2, device_id=(0, self.c, peer), device_id_type=MESH).start()
                return 0
            lax.fori_loop(1, NCH, send, 0)
            self.o[dst] = t[0]

    def gather(self):
        @pl.when(self.unit < self.U)
        def _():
            self.rows(self.U - 1, self.s2, self.r2).wait_recv()

        @pl.when(self.unit >= self.U)
        def _():
            self.rows(self.U, self.s2, self.r2).wait_recv()
        self.exch(self.o, self.o.at[self.mine], self.s3, self.r3, self.mine).start()

    def finish(self, g):
        self.exch(self.o, self.o.at[self.mine], self.s3, self.r3, self.mine).wait_recv()
        for n, (i, j) in enumerate(BLKS[self.ch]):
            g[rb(i), rb(j)] = self.o[rb(n), :]

    def drain(self):
        self.exch(self.p, self.recv0, self.s0, self.r0, self.mine).wait_send()
        self.exch(self.o, self.o.at[self.mine], self.s3, self.r3, self.mine).wait_send()

        @pl.when(self.unit < self.U)
        def _():
            self.rows(self.U - 1, self.s1, self.r1).wait_send()
            self.rows(63, self.s2, self.r2).wait_send()

        @pl.when(self.unit >= self.U)
        def _():
            self.rows(self.U, self.s1, self.r1).wait_send()


def greet(c, me):
    bar = pltpu.get_barrier_semaphore()
    pl.semaphore_signal(bar, inc=1, device_id=(0, 1 - c, me), device_id_type=MESH)

    def sig(k, _):
        pl.semaphore_signal(bar, inc=1, device_id=(0, c, lax.rem(me + k, NCH)), device_id_type=MESH)
        return 0
    lax.fori_loop(1, NCH, sig, 0)
    return bar


def eliminate(j, a, b, g, l, m):
    if a < b:
        v = dot(g[rb(a, b), rb(j)], m[rb(j), rb(j)], NT)
        l[rb(a, b), rb(j)] = v
        g[rb(a, b), rb(j + 1, b)] = g[rb(a, b), rb(j + 1, b)] - dot(v, l[rb(j + 1, b), rb(j)], NT)


def apply_cols(x_ref, m_ref, q_ref, a, b):
    def rows(r, _):
        sl = pl.ds(pl.multiple_of(256 * r, 256), 256)
        q_ref[sl, rb(a, b)] = dot(x_ref[sl, rb(0, b)], m_ref[rb(a, b), rb(0, b)], NT)
        return 0
    lax.fori_loop(0, x_ref.shape[0] // 256, rows, 0)


JOIN = ((-1, 1, 2, 2), (5, 7, 8, 10))
GATHER = ((-1, 0, 1, 1), (4, 6, 7, 9))
REDUCE = ((-1, -1, -1, 0), (3, 5, 6, 8))
SCATTER = ((-1, -1, -1, -1), (2, 4, 5, 6))
APPLY = {1: 0, 3: 1, 4: 2, 5: 3}


def main_kernel(x, q, m2, l1, l2, g, m1, dbuf, ubuf, mbuf, *rest):
    c, me = lax.axis_index("outer"), lax.axis_index("rows")
    bar = greet(c, me)
    nc = len(CHUNKS)
    bufs, sems = rest[:12 * nc], rest[12 * nc:]
    S = [[Sum(ch, c, me, bufs[6 * (nc * s + ch):6 * (nc * s + ch) + 6], [r.at[s, ch] for r in sems]) for ch in range(nc)] for s in range(2)]
    S0, S1 = S
    for r in (m1, m2, l1, l2):
        r[...] = jnp.zeros_like(r)
    S0[0].gram(x)
    S0[1].gram(x)
    pl.semaphore_wait(bar, NCH)
    S0[0].swap()
    S0[1].swap()
    S0[2].gram(x)
    S0[2].swap()
    S0[0].scatter()
    S0[1].scatter()
    S0[3].gram(x)
    S0[3].swap()
    S0[2].scatter()
    S0[0].reduce()
    S0[3].scatter()
    S0[1].reduce()
    S0[2].reduce()
    S0[0].gather()
    S0[0].finish(g)
    dbuf[...] = g[rb(0), rb(0)]

    def section(t):
        s, k = divmod(t, NB)
        l, m = ((l1, m1), (l2, m2))[s]
        for ss in range(2):
            for ch in range(nc):
                if SCATTER[ss][ch] == t:
                    S[ss][ch].scatter()
        for ss in range(2):
            for ch in range(nc):
                if REDUCE[ss][ch] == t:
                    S[ss][ch].reduce()
        for ss in range(2):
            for ch in range(nc):
                if GATHER[ss][ch] == t:
                    S[ss][ch].gather()
        m[rb(k), rb(k)] = mbuf[...]
        l[rb(k), rb(k)] = ubuf[...].T
        end = max(CHUNKS[ch][1] for ch in range(nc) if JOIN[s][ch] < t)
        eliminate(k, k + 1, end, g, l, m)
        for ch in range(nc):
            if JOIN[s][ch] == t:
                S[s][ch].finish(g)
                a, b, _ = CHUNKS[ch]
                for j in range(k + 1):
                    eliminate(j, a, b, g, l, m)
        if k < NB - 1:
            dbuf[...] = g[rb(k + 1), rb(k + 1)]
        if k > 0:
            m[rb(k), rb(0, k)] = -dot(mbuf[...], dot(l[rb(k), rb(0, k)], m[rb(0, k), rb(0, k)], ((1,), (0,))), ((1,), (0,)))
        if t in APPLY:
            ch = APPLY[t]
            a, b, _ = CHUNKS[ch]
            apply_cols(x, m, q, a, b)
            S1[ch].gram(q)
            S1[ch].swap()
        if t == NB - 1:
            S1[0].finish(g)
            dbuf[...] = g[rb(0), rb(0)]

    def step(t, _):
        factor(dbuf, ubuf, mbuf)
        for tt in range(2 * NB):
            @pl.when(t == tt)
            def _():
                section(tt)
        return 0

    lax.fori_loop(0, 2 * NB, step, 0)
    for s in S:
        for ch in s:
            ch.drain()


def last_kernel(x, m, l2, l1, q, r):
    for j in range(3):
        apply_cols(x, m, q, 2 * j, 2 * j + 2)
    for i in range(3):
        for j in range(3):
            a, b = rb(2 * i, 2 * i + 2), rb(2 * j, 2 * j + 2)
            if i > j:
                r[a, b] = jnp.zeros((256, 256), jnp.float32)
            else:
                k = rb(2 * i, 2 * j + 2)
                r[a, b] = dot(l2[k, a], l1[b, k], ((0,), (1,)))


def solution(mesh):
    spec = P(("batch", "outer", "rows"), None)
    V = pl.BlockSpec(memory_space=pltpu.VMEM)
    F = lambda *s: jax.ShapeDtypeStruct(s, jnp.float32)
    B = lambda *s: pltpu.VMEM(s, jnp.float32)
    bufs = []
    for u in 2 * UNITS:
        bufs += [B(16 * u, 128), B(8 * u, 128), B(8 * u, 128), B(504, 128), B(16 * u, 128), B(8, 128)]

    def local_qr(a):
        q1, m2, l1, l2 = pl.pallas_call(
            main_kernel, out_shape=(F(*a.shape), F(N, N), F(N, N), F(N, N)), in_specs=[V], out_specs=(V,) * 4,
            scratch_shapes=[B(N, N), B(N, N), B(128, 128), B(128, 128), B(128, 128)] + bufs + [pltpu.SemaphoreType.DMA((2, len(CHUNKS)))] * 8,
            compiler_params=pltpu.CompilerParams(vmem_limit_bytes=56 * 2**20, collective_id=0, has_side_effects=True), name="sweeps")(a)
        return tuple(pl.pallas_call(
            last_kernel, out_shape=(F(*a.shape), F(N, N)), in_specs=[V] * 4, out_specs=(V, V),
            compiler_params=pltpu.CompilerParams(vmem_limit_bytes=40 * 2**20), name="last")(q1, m2, l2, l1))

    return jax.shard_map(local_qr, mesh=mesh, in_specs=(spec,), out_specs=(spec, P("batch", None)), check_vma=False)
```

```python
import jax
import jax.numpy as jnp
from jax import lax
from jax.experimental import pallas as pl
from jax.experimental.pallas import tpu as pltpu
from jax.sharding import PartitionSpec as P

MESH = pl.DeviceIdType.MESH
HI = lax.Precision.HIGHEST
NT = ((1,), (1,))
N = 768
NB = 6
NCH = 64
CHUNKS = ((0, 2, 0), (2, 4, 24), (4, 5, 16), (5, 6, 56))
BLKS = tuple(tuple((i, j) for i in range(a, b) for j in range(i + 1)) for a, b, _ in CHUNKS)
UNITS = tuple(8 * len(b) for b in BLKS)


def dot(a, b, dims):
    return lax.dot_general(a, b, (dims, ((), ())), precision=HI, preferred_element_type=jnp.float32)


def m8(v):
    return pl.multiple_of(v, 8)


def rb(i, j=None):
    return slice(128 * i, 128 * (i + 1 if j is None else j))


def bl(x, l):
    return jnp.broadcast_to(x[:, l:l + 1], (8, 128))

def bs(x, s):
    return jnp.broadcast_to(x[s:s + 1, :], (8, 128))

def factor(dref, uref, mref):
    sub = lax.broadcasted_iota(jnp.int32, (8, 128), 0)
    lane = lax.broadcasted_iota(jnp.int32, (8, 128), 1)
    zero = jnp.zeros((8, 128), jnp.float32)
    A = [dref[8 * i:8 * i + 8, :] for i in range(16)]
    for sp in range(8):
        l0 = 16 * sp
        ia, ib = 2 * sp, 2 * sp + 1
        blk = (lane >= l0) & (lane < l0 + 16)
        Ua, Ub = A[ia], A[ib]
        ca = [bl(Ua, l0 + s) for s in range(8)]
        cb = [bl(Ub, l0 + s) for s in range(16)]
        urg = [n for n in (ia + 2, ia + 3) if n < 16]
        cn = {n: [bl(A[n], l0 + s) for s in range(16)] for n in urg}
        Wa = jnp.where(blk, jnp.where(lane == sub + l0, 1.0, zero), Ua)
        Wb = jnp.where(blk, jnp.where(lane == sub + (l0 + 8), 1.0, zero), Ub)
        for n in range(ia + 2, 16):
            A[n] = jnp.where(blk, zero, A[n])
        for s in range(16):
            first = s < 8
            r = s % 8
            ri = lax.rsqrt(bs(ca[s] if first else cb[s], r))
            lb = cb[s] * ri
            if first:
                la = ca[s] * ri
                L = {t: (bs(la, t) if t < 8 else bs(lb, t - 8)) for t in range(s + 1, 16)}
                for t in range(s + 1, 8):
                    ca[t] = ca[t] - la * L[t]
                ma = jnp.where(sub > r, la, zero)
                u, w = bs(Ua, r) * ri, bs(Wa, r) * ri
                Ua = jnp.where(sub == r, u, Ua - ma * u)
                Wa = jnp.where(sub == r, w, Wa - ma * w)
                Ub = Ub - lb * u
                Wb = Wb - lb * w
            else:
                L = {t: bs(lb, t - 8) for t in range(s + 1, 16)}
                mb = jnp.where(sub > r, lb, zero)
                u, w = bs(Ub, r) * ri, bs(Wb, r) * ri
                Ub = jnp.where(sub == r, u, Ub - mb * u)
                Wb = jnp.where(sub == r, w, Wb - mb * w)
            for t in range(s + 1, 16):
                cb[t] = cb[t] - lb * L[t]
            for n in urg:
                ln = cn[n][s] * ri
                for t in range(s + 1, 16):
                    cn[n][t] = cn[n][t] - ln * L[t]
                A[n] = A[n] - ln * w
        uref[l0:l0 + 8, :] = jnp.where(lane >= sub + l0, Ua, zero)
        uref[l0 + 8:l0 + 16, :] = jnp.where(lane >= sub + (l0 + 8), Ub, zero)
        keep = lane < l0 + 16
        mref[l0:l0 + 8, :] = jnp.where(keep, Wa, zero)
        mref[l0 + 8:l0 + 16, :] = jnp.where(keep, Wb, zero)
        if ia + 4 < 16:
            W = jnp.concatenate([Wa, Wb], axis=0)
            D = dot(W, W, ((0,), (0,)))
            for n in range(ia + 4, 16):
                A[n] = A[n] - D[8 * n:8 * n + 8, :]


class Sum:
    def __init__(self, ch, c, me, bufs, sems):
        self.ch, self.c, self.me, self.other = ch, c, me, 1 - c
        self.p, self.recv0, self.acc, self.recv1, self.o, self.red = bufs
        self.s0, self.r0, self.s1, self.r1, self.s2, self.r2, self.s3, self.r3 = sems
        self.U = UNITS[ch]
        self.half = 8 * self.U
        self.base = CHUNKS[ch][2]
        self.mine = pl.ds(m8(c * self.half), self.half)
        self.unit = lax.rem(me - self.base + NCH, NCH)

    def gram(self, x):
        a, b, _ = CHUNKS[self.ch]
        full = dot(x[:, rb(a, b)], x[:, rb(0, b)], ((0,), (0,)))
        for n, (i, j) in enumerate(BLKS[self.ch]):
            self.p[rb(n), :] = full[rb(i - a), rb(j)]

    def exch(self, ref, dst, s, r, sl):
        return pltpu.make_async_remote_copy(ref.at[sl], dst, s, r, device_id=(0, self.other, self.me), device_id_type=MESH)

    def swap(self):
        sl = pl.ds(m8(self.other * self.half), self.half)
        self.cp0 = self.exch(self.p, self.recv0, self.s0, self.r0, sl)
        self.cp0.start()

    def scatter(self):
        self.exch(self.p, self.recv0, self.s0, self.r0, self.mine).wait_recv()
        self.acc[...] = self.p[self.mine] + self.recv0[...]

        def send(i, _):
            u = lax.rem(self.me + i, self.U)
            peer = lax.rem(self.base + u, NCH)
            k = lax.rem(peer - self.me + NCH, NCH)

            @pl.when(k > 0)
            def _():
                pltpu.make_async_remote_copy(self.acc.at[pl.ds(m8(8 * u), 8)], self.recv1.at[pl.ds(m8(8 * k - 8), 8)], self.s1, self.r1, device_id=(0, self.c, peer), device_id_type=MESH).start()
            return 0
        lax.fori_loop(0, self.U, send, 0)

    def rows(self, n, s, r):
        return pltpu.make_async_remote_copy(self.recv1.at[pl.ds(0, 8 * n)], self.recv1.at[pl.ds(0, 8 * n)], s, r, device_id=(0, self.other, self.me), device_id_type=MESH)

    def reduce(self):
        @pl.when(self.unit < self.U)
        def _():
            self.rows(63, self.s1, self.r1).wait_recv()
            t = [self.acc[pl.ds(m8(8 * self.unit), 8)]] + [self.recv1[8 * k:8 * k + 8, :] for k in range(63)]
            while len(t) > 1:
                t = [t[i] + t[i + 1] for i in range(0, len(t), 2)]
            self.red[...] = t[0]
            dst = pl.ds(m8(self.c * self.half + 8 * self.unit), 8)

            def send(k, _):
                peer = lax.rem(self.me + k, NCH)
                pltpu.make_async_remote_copy(self.red, self.o.at[dst], self.s2, self.r2, device_id=(0, self.c, peer), device_id_type=MESH).start()
                return 0
            lax.fori_loop(1, NCH, send, 0)
            self.o[dst] = t[0]

    def gather(self):
        @pl.when(self.unit < self.U)
        def _():
            self.rows(self.U - 1, self.s2, self.r2).wait_recv()

        @pl.when(self.unit >= self.U)
        def _():
            self.rows(self.U, self.s2, self.r2).wait_recv()
        self.exch(self.o, self.o.at[self.mine], self.s3, self.r3, self.mine).start()

    def finish(self, g):
        self.exch(self.o, self.o.at[self.mine], self.s3, self.r3, self.mine).wait_recv()
        for n, (i, j) in enumerate(BLKS[self.ch]):
            g[rb(i), rb(j)] = self.o[rb(n), :]

    def drain(self):
        self.exch(self.p, self.recv0, self.s0, self.r0, self.mine).wait_send()
        self.exch(self.o, self.o.at[self.mine], self.s3, self.r3, self.mine).wait_send()

        @pl.when(self.unit < self.U)
        def _():
            self.rows(self.U - 1, self.s1, self.r1).wait_send()
            self.rows(63, self.s2, self.r2).wait_send()

        @pl.when(self.unit >= self.U)
        def _():
            self.rows(self.U, self.s1, self.r1).wait_send()


def greet(c, me):
    bar = pltpu.get_barrier_semaphore()
    pl.semaphore_signal(bar, inc=1, device_id=(0, 1 - c, me), device_id_type=MESH)

    def sig(k, _):
        pl.semaphore_signal(bar, inc=1, device_id=(0, c, lax.rem(me + k, NCH)), device_id_type=MESH)
        return 0
    lax.fori_loop(1, NCH, sig, 0)
    return bar


def eliminate(j, a, b, g, l, w):
    if a < b:
        v = dot(g[rb(a, b), rb(j)], w[rb(j), wl(j)], NT)
        l[rb(a, b), rb(j)] = v
        for m in range(j + 1, b, 2):
            lo, hi = max(a, m), min(m + 2, b)
            g[rb(lo, b), rb(m, hi)] = g[rb(lo, b), rb(m, hi)] - dot(v[128 * (lo - a):, :], l[rb(m, hi), rb(j)], NT)


def wl(k):
    return rb(k % 2)


def pair(k, l, w):
    w[rb(k), rb(0)] = -dot(w[rb(k), rb(1)], dot(l[rb(k), rb(k - 1)], w[rb(k - 1), rb(0)], ((1,), (0,))), ((1,), (0,)))


def solve_cols(x_ref, l, w, q_ref, a, b, step=256):
    def rows(r, _):
        sl = pl.ds(pl.multiple_of(step * r, step), step)
        t = x_ref[sl, rb(a, b)]
        if a:
            t = t - dot(q_ref[sl, rb(0, a)], l[rb(a, b), rb(0, a)], NT)
        q_ref[sl, rb(a, b)] = dot(t, w[rb(a, b), :] if b - a == 2 else w[rb(a), wl(a)], NT)
        return 0
    lax.fori_loop(0, x_ref.shape[0] // step, rows, 0)


JOIN = ((-1, 1, 2, 2), (5, 7, 8, 10))
GATHER = ((-1, 0, 1, 1), (4, 6, 7, 9))
REDUCE = ((-1, -1, -1, 0), (3, 5, 6, 8))
SCATTER = ((-1, -1, -1, -1), (2, 4, 5, 6))
APPLY = {1: 0, 3: 1, 4: 2, 5: 3}


def main_kernel(x, q, w2, l1, l2, g, w1, dbuf, ubuf, mbuf, *rest):
    c, me = lax.axis_index("outer"), lax.axis_index("rows")
    bar = greet(c, me)
    nc = len(CHUNKS)
    bufs, sems = rest[:12 * nc], rest[12 * nc:]
    S = [[Sum(ch, c, me, bufs[6 * (nc * s + ch):6 * (nc * s + ch) + 6], [r.at[s, ch] for r in sems]) for ch in range(nc)] for s in range(2)]
    S0, S1 = S
    for r in (w1, w2, l1, l2):
        r[...] = jnp.zeros_like(r)
    S0[0].gram(x)
    S0[1].gram(x)
    pl.semaphore_wait(bar, NCH)
    S0[0].swap()
    S0[1].swap()
    S0[2].gram(x)
    S0[2].swap()
    S0[0].scatter()
    S0[1].scatter()
    S0[3].gram(x)
    S0[3].swap()
    S0[2].scatter()
    S0[0].reduce()
    S0[3].scatter()
    S0[1].reduce()
    S0[2].reduce()
    S0[0].gather()
    S0[0].finish(g)
    dbuf[...] = g[rb(0), rb(0)]

    def section(t):
        s, k = divmod(t, NB)
        l, w = ((l1, w1), (l2, w2))[s]
        for ss in range(2):
            for ch in range(nc):
                if SCATTER[ss][ch] == t:
                    S[ss][ch].scatter()
        for ss in range(2):
            for ch in range(nc):
                if REDUCE[ss][ch] == t:
                    S[ss][ch].reduce()
        for ss in range(2):
            for ch in range(nc):
                if GATHER[ss][ch] == t:
                    S[ss][ch].gather()
        w[rb(k), wl(k)] = mbuf[...]
        l[rb(k), rb(k)] = ubuf[...].T
        end = max(CHUNKS[ch][1] for ch in range(nc) if JOIN[s][ch] < t)
        eliminate(k, k + 1, end, g, l, w)
        for ch in range(nc):
            if JOIN[s][ch] == t:
                S[s][ch].finish(g)
                a, b, _ = CHUNKS[ch]
                for j in range(k + 1):
                    eliminate(j, a, b, g, l, w)
        if k < NB - 1:
            dbuf[...] = g[rb(k + 1), rb(k + 1)]
        if k % 2:
            pair(k, l, w)
        if t in APPLY:
            ch = APPLY[t]
            a, b, _ = CHUNKS[ch]
            solve_cols(x, l, w, q, a, b)
            S1[ch].gram(q)
            S1[ch].swap()
        if t == NB - 1:
            S1[0].finish(g)
            dbuf[...] = g[rb(0), rb(0)]

    def step(t, _):
        factor(dbuf, ubuf, mbuf)
        for tt in range(2 * NB):
            @pl.when(t == tt)
            def _():
                section(tt)
        return 0

    lax.fori_loop(0, 2 * NB, step, 0)
    for s in S:
        for ch in s:
            ch.drain()


def last_kernel(x, w, l2, l1, q, r):
    for j in range(3):
        solve_cols(x, l2, w, q, 2 * j, 2 * j + 2)
    for i in range(3):
        for j in range(i):
            r[rb(2 * i, 2 * i + 2), rb(2 * j, 2 * j + 2)] = jnp.zeros((256, 256), jnp.float32)

    def blk(i):
        return pl.ds(pl.multiple_of(256 * i, 256), 256)

    def diag(w):
        def f(i, _):
            k = pl.ds(pl.multiple_of(256 * i, 256), 256 * (w + 1))
            r[blk(i), blk(i + w)] = dot(l2[k, blk(i)], l1[blk(i + w), k], ((0,), (1,)))
            return 0
        lax.fori_loop(0, 3 - w, f, 0)
    for w in range(3):
        diag(w)


def solution(mesh):
    spec = P(("batch", "outer", "rows"), None)
    V = pl.BlockSpec(memory_space=pltpu.VMEM)
    F = lambda *s: jax.ShapeDtypeStruct(s, jnp.float32)
    B = lambda *s: pltpu.VMEM(s, jnp.float32)
    bufs = []
    for u in 2 * UNITS:
        bufs += [B(16 * u, 128), B(8 * u, 128), B(8 * u, 128), B(504, 128), B(16 * u, 128), B(8, 128)]

    def local_qr(a):
        q1, w2, l1, l2 = pl.pallas_call(
            main_kernel, out_shape=(F(*a.shape), F(N, 256), F(N, N), F(N, N)), in_specs=[V], out_specs=(V,) * 4,
            scratch_shapes=[B(N, N), B(N, 256), B(128, 128), B(128, 128), B(128, 128)] + bufs + [pltpu.SemaphoreType.DMA((2, len(CHUNKS)))] * 8,
            compiler_params=pltpu.CompilerParams(vmem_limit_bytes=34 * 2**20, collective_id=0, has_side_effects=True), name="sweeps")(a)
        return tuple(pl.pallas_call(
            last_kernel, out_shape=(F(*a.shape), F(N, N)), in_specs=[V] * 4, out_specs=(V, V),
            compiler_params=pltpu.CompilerParams(vmem_limit_bytes=20 * 2**20), name="last")(q1, w2, l2, l1))

    return jax.shard_map(local_qr, mesh=mesh, in_specs=(spec,), out_specs=(spec, P("batch", None)), check_vma=False)
```

```python
import jax
import jax.numpy as jnp
from jax import lax
from jax.experimental import pallas as pl
from jax.experimental.pallas import tpu as pltpu
from jax.sharding import PartitionSpec as P

MESH = pl.DeviceIdType.MESH
HI = lax.Precision.HIGHEST
NT = ((1,), (1,))
N = 768
NB = 6
NCH = 64
CHUNKS = ((0, 2, 0), (2, 4, 12), (4, 5, 40), (5, 6, 60))
BLKS = tuple(tuple((i, j) for i in range(a, b) for j in range(i + 1)) for a, b, _ in CHUNKS)
UT = 16
UNITS = tuple(64 * len(b) // UT for b in BLKS)


def dot(a, b, dims):
    return lax.dot_general(a, b, (dims, ((), ())), precision=HI, preferred_element_type=jnp.float32)


def m8(v):
    return pl.multiple_of(v, 8)


def wrap(v):
    return jnp.where(v >= NCH, v - NCH, v)


def rb(i, j=None):
    return slice(128 * i, 128 * (i + 1 if j is None else j))


def bl(x, l):
    return jnp.broadcast_to(x[:, l:l + 1], (8, 128))

def bs(x, s):
    return jnp.broadcast_to(x[s:s + 1, :], (8, 128))

def factor(dref, uref, mref):
    sub = lax.broadcasted_iota(jnp.int32, (8, 128), 0)
    lane = lax.broadcasted_iota(jnp.int32, (8, 128), 1)
    zero = jnp.zeros((8, 128), jnp.float32)
    A = [dref[8 * i:8 * i + 8, :] for i in range(16)]
    for sp in range(8):
        l0 = 16 * sp
        ia, ib = 2 * sp, 2 * sp + 1
        blk = (lane >= l0) & (lane < l0 + 16)
        Ua, Ub = A[ia], A[ib]
        ca = [bl(Ua, l0 + s) for s in range(8)]
        cb = [bl(Ub, l0 + s) for s in range(16)]
        urg = [n for n in (ia + 2, ia + 3) if n < 16]
        cn = {n: [bl(A[n], l0 + s) for s in range(16)] for n in urg}
        Wa = jnp.where(blk, jnp.where(lane == sub + l0, 1.0, zero), Ua)
        Wb = jnp.where(blk, jnp.where(lane == sub + (l0 + 8), 1.0, zero), Ub)
        for n in range(ia + 2, 16):
            A[n] = jnp.where(blk, zero, A[n])
        for s in range(16):
            first = s < 8
            r = s % 8
            ri = lax.rsqrt(bs(ca[s] if first else cb[s], r))
            lb = cb[s] * ri
            if first:
                la = ca[s] * ri
                L = {t: (bs(la, t) if t < 8 else bs(lb, t - 8)) for t in range(s + 1, 16)}
                for t in range(s + 1, 8):
                    ca[t] = ca[t] - la * L[t]
                ma = jnp.where(sub > r, la, zero)
                u, w = bs(Ua, r) * ri, bs(Wa, r) * ri
                Ua = jnp.where(sub == r, u, Ua - ma * u)
                Wa = jnp.where(sub == r, w, Wa - ma * w)
                Ub = Ub - lb * u
                Wb = Wb - lb * w
            else:
                L = {t: bs(lb, t - 8) for t in range(s + 1, 16)}
                mb = jnp.where(sub > r, lb, zero)
                u, w = bs(Ub, r) * ri, bs(Wb, r) * ri
                Ub = jnp.where(sub == r, u, Ub - mb * u)
                Wb = jnp.where(sub == r, w, Wb - mb * w)
            for t in range(s + 1, 16):
                cb[t] = cb[t] - lb * L[t]
            for n in urg:
                ln = cn[n][s] * ri
                for t in range(s + 1, 16):
                    cn[n][t] = cn[n][t] - ln * L[t]
                A[n] = A[n] - ln * w
        uref[l0:l0 + 8, :] = jnp.where(lane >= sub + l0, Ua, zero)
        uref[l0 + 8:l0 + 16, :] = jnp.where(lane >= sub + (l0 + 8), Ub, zero)
        keep = lane < l0 + 16
        mref[l0:l0 + 8, :] = jnp.where(keep, Wa, zero)
        mref[l0 + 8:l0 + 16, :] = jnp.where(keep, Wb, zero)
        if ia + 4 < 16:
            W = jnp.concatenate([Wa, Wb], axis=0)
            D = dot(W, W, ((0,), (0,)))
            for n in range(ia + 4, 16):
                A[n] = A[n] - D[8 * n:8 * n + 8, :]


class Sum:
    def __init__(self, ch, c, me, bufs, sems):
        self.ch, self.c, self.me, self.other = ch, c, me, 1 - c
        self.p, self.recv0, self.acc, self.recv1, self.o, self.red = bufs
        self.s0, self.r0, self.s1, self.r1, self.s2, self.r2, self.s3, self.r3 = sems
        self.U = UNITS[ch]
        self.half = UT * self.U
        self.base = wrap(CHUNKS[ch][2] + 32 * c)
        self.mine = pl.ds(m8(c * self.half), self.half)
        self.unit = wrap(me - self.base + NCH)

    def gram(self, x):
        a, b, _ = CHUNKS[self.ch]
        full = dot(x[:, rb(a, b)], x[:, rb(0, b)], ((0,), (0,)))
        for n, (i, j) in enumerate(BLKS[self.ch]):
            self.p[rb(n), :] = full[rb(i - a), rb(j)]

    def exch(self, ref, dst, s, r, sl):
        return pltpu.make_async_remote_copy(ref.at[sl], dst, s, r, device_id=(0, self.other, self.me), device_id_type=MESH)

    def swap(self):
        sl = pl.ds(m8(self.other * self.half), self.half)
        self.cp0 = self.exch(self.p, self.recv0, self.s0, self.r0, sl)
        self.cp0.start()

    def scatter(self):
        self.exch(self.p, self.recv0, self.s0, self.r0, self.mine).wait_recv()
        self.acc[...] = self.p[self.mine] + self.recv0[...]
        slot = pl.ds(m8(UT * self.me), UT)
        first = lax.rem(self.me, self.U)

        def send(i, _):
            u = first + i
            u = jnp.where(u >= self.U, u - self.U, u)
            peer = wrap(self.base + u)

            @pl.when(peer != self.me)
            def _():
                pltpu.make_async_remote_copy(self.acc.at[pl.ds(m8(UT * u), UT)], self.recv1.at[slot], self.s1, self.r1, device_id=(0, self.c, peer), device_id_type=MESH).start()
            return 0
        lax.fori_loop(0, self.U, send, 0, unroll=4)

    def rows(self, n, s, r):
        return pltpu.make_async_remote_copy(self.recv1.at[pl.ds(0, UT * n)], self.recv1.at[pl.ds(0, UT * n)], s, r, device_id=(0, self.other, self.me), device_id_type=MESH)

    def reduce(self):
        @pl.when(self.unit < self.U)
        def _():
            self.recv1[pl.ds(m8(UT * self.me), UT)] = self.acc[pl.ds(m8(UT * self.unit), UT)]
            self.rows(63, self.s1, self.r1).wait_recv()
            t = [self.recv1[UT * k:UT * k + UT, :] for k in range(NCH)]
            while len(t) > 1:
                t = [t[i] + t[i + 1] for i in range(0, len(t), 2)]
            self.red[...] = t[0]
            dst = pl.ds(m8(self.c * self.half + UT * self.unit), UT)

            def send(k, _):
                pltpu.make_async_remote_copy(self.red, self.o.at[dst], self.s2, self.r2, device_id=(0, self.c, wrap(self.me + k)), device_id_type=MESH).start()
                return 0
            lax.fori_loop(1, NCH, send, 0, unroll=7)
            self.o[dst] = t[0]

    def gather(self):
        @pl.when(self.unit < self.U)
        def _():
            self.rows(self.U - 1, self.s2, self.r2).wait_recv()

        @pl.when(self.unit >= self.U)
        def _():
            self.rows(self.U, self.s2, self.r2).wait_recv()
        self.exch(self.o, self.o.at[self.mine], self.s3, self.r3, self.mine).start()

    def finish(self, g):
        self.exch(self.o, self.o.at[self.mine], self.s3, self.r3, self.mine).wait_recv()
        for n, (i, j) in enumerate(BLKS[self.ch]):
            g[rb(i), rb(j)] = self.o[rb(n), :]

    def drain(self):
        self.exch(self.p, self.recv0, self.s0, self.r0, self.mine).wait_send()
        self.exch(self.o, self.o.at[self.mine], self.s3, self.r3, self.mine).wait_send()

        @pl.when(self.unit < self.U)
        def _():
            self.rows(self.U - 1, self.s1, self.r1).wait_send()
            self.rows(63, self.s2, self.r2).wait_send()

        @pl.when(self.unit >= self.U)
        def _():
            self.rows(self.U, self.s1, self.r1).wait_send()


def greet(c, me):
    bar = pltpu.get_barrier_semaphore()
    pl.semaphore_signal(bar, inc=1, device_id=(0, 1 - c, me), device_id_type=MESH)

    def sig(k, _):
        pl.semaphore_signal(bar, inc=1, device_id=(0, c, wrap(me + k)), device_id_type=MESH)
        return 0
    lax.fori_loop(1, NCH, sig, 0, unroll=7)
    return bar


def eliminate(j, a, b, g, l, w):
    if a < b:
        v = dot(g[rb(a, b), rb(j)], w[rb(j), wl(j)], NT)
        l[rb(a, b), rb(j)] = v
        for m in range(j + 1, b, 2):
            lo, hi = max(a, m), min(m + 2, b)
            g[rb(lo, b), rb(m, hi)] = g[rb(lo, b), rb(m, hi)] - dot(v[128 * (lo - a):, :], l[rb(m, hi), rb(j)], NT)


def wl(k):
    return rb(k % 2)


def pair(k, l, w):
    w[rb(k), rb(0)] = -dot(w[rb(k), rb(1)], dot(l[rb(k), rb(k - 1)], w[rb(k - 1), rb(0)], ((1,), (0,))), ((1,), (0,)))


def solve_rows(x_ref, l, w, q_ref, a, b, sl):
    t = x_ref[sl, rb(a, b)]
    if a:
        t = t - dot(q_ref[sl, rb(0, a)], l[rb(a, b), rb(0, a)], NT)
    q_ref[sl, rb(a, b)] = dot(t, w[rb(a, b), :] if b - a == 2 else w[rb(a), wl(a)], NT)


def solve_cols(x_ref, l, w, q_ref, a, b):
    def rows(r, _):
        solve_rows(x_ref, l, w, q_ref, a, b, pl.ds(pl.multiple_of(256 * r, 256), 256))
        return 0
    lax.fori_loop(0, x_ref.shape[0] // 256, rows, 0)


JOIN = ((-1, 1, 2, 2), (5, 7, 9, 10))
GATHER = ((-1, 0, 1, 1), (4, 7, 9, 10))
REDUCE = ((-1, -1, -1, 0), (3, 5, 7, 8))
SCATTER = ((-1, -1, -1, -1), (2, 4, 5, 6))
APPLY = {1: 0, 3: 1, 4: 2, 5: 3}


def main_kernel(x, q, w2, l1, l2, g, w1, dbuf, ubuf, mbuf, *rest):
    c, me = lax.axis_index("outer"), lax.axis_index("rows")
    bar = greet(c, me)
    nc = len(CHUNKS)
    bufs, sems = rest[:12 * nc], rest[12 * nc:]
    S = [[Sum(ch, c, me, bufs[6 * (nc * s + ch):6 * (nc * s + ch) + 6], [r.at[s, ch] for r in sems]) for ch in range(nc)] for s in range(2)]
    S0, S1 = S
    for r in (w1, w2, l1, l2):
        r[...] = jnp.zeros_like(r)
    for ch in range(3):
        S0[ch].gram(x)
    pl.semaphore_wait(bar, NCH)
    for ch in range(3):
        S0[ch].swap()
    for ch in range(2):
        S0[ch].scatter()
    S0[3].gram(x)
    S0[3].swap()
    for ch in (2, 3):
        S0[ch].scatter()
    for ch in range(3):
        S0[ch].reduce()
    S0[0].gather()
    S0[0].finish(g)
    dbuf[...] = g[rb(0), rb(0)]

    def section(t):
        s, k = divmod(t, NB)
        l, w = ((l1, w1), (l2, w2))[s]
        for ss in range(2):
            for ch in range(nc):
                if SCATTER[ss][ch] == t:
                    S[ss][ch].scatter()
        for ss in range(2):
            for ch in range(nc):
                if REDUCE[ss][ch] == t:
                    S[ss][ch].reduce()
        for ss in range(2):
            for ch in range(nc):
                if GATHER[ss][ch] == t:
                    S[ss][ch].gather()
        w[rb(k), wl(k)] = mbuf[...]
        l[rb(k), rb(k)] = ubuf[...].T
        end = max(CHUNKS[ch][1] for ch in range(nc) if JOIN[s][ch] < t)
        eliminate(k, k + 1, end, g, l, w)
        for ch in range(nc):
            if JOIN[s][ch] == t:
                S[s][ch].finish(g)
                a, b, _ = CHUNKS[ch]
                for j in range(k + 1):
                    eliminate(j, a, b, g, l, w)
        if k < NB - 1:
            dbuf[...] = g[rb(k + 1), rb(k + 1)]
        if k % 2:
            pair(k, l, w)
        if t in APPLY:
            ch = APPLY[t]
            a, b, _ = CHUNKS[ch]
            solve_cols(x, l, w, q, a, b)
            S1[ch].gram(q)
            S1[ch].swap()
        if t == NB - 1:
            S1[0].finish(g)
            dbuf[...] = g[rb(0), rb(0)]

    def step(t, _):
        factor(dbuf, ubuf, mbuf)
        for tt in range(2 * NB):
            @pl.when(t == tt)
            def _():
                section(tt)
        return 0

    lax.fori_loop(0, 2 * NB, step, 0)
    for s in S:
        for ch in s:
            ch.drain()


def last_kernel(x, w, l2, l1, qo, ro, q, r, sem):
    def blk(i):
        return pl.ds(pl.multiple_of(256 * i, 256), 256)

    for i in range(3):
        for j in range(i):
            r[rb(2 * i, 2 * i + 2), rb(2 * j, 2 * j + 2)] = jnp.zeros((256, 256), jnp.float32)

    def diag(d):
        def f(i, _):
            k = pl.ds(pl.multiple_of(256 * i, 256), 256 * (d + 1))
            r[blk(i), blk(i + d)] = dot(l2[k, blk(i)], l1[blk(i + d), k], ((0,), (1,)))
            return 0
        lax.fori_loop(0, 3 - d, f, 0)
    for d in range(3):
        diag(d)
    out = pltpu.make_async_copy(r, ro, sem.at[0])
    out.start()
    half = x.shape[0] // 2

    def rows(h, _):
        sl = pl.ds(pl.multiple_of(half * h, half), half)
        for j in range(3):
            solve_rows(x, l2, w, q, 2 * j, 2 * j + 2, sl)
        pltpu.make_async_copy(q.at[sl], qo.at[sl], sem.at[h + 1]).start()
        return 0
    lax.fori_loop(0, 2, rows, 0)
    for h in range(2):
        sl = pl.ds(half * h, half)
        pltpu.make_async_copy(q.at[sl], qo.at[sl], sem.at[h + 1]).wait()
    out.wait()


def solution(mesh):
    spec = P(("batch", "outer", "rows"), None)
    V = pl.BlockSpec(memory_space=pltpu.VMEM)
    H = pl.BlockSpec(memory_space=pl.ANY)
    F = lambda *s: jax.ShapeDtypeStruct(s, jnp.float32)
    B = lambda *s: pltpu.VMEM(s, jnp.float32)
    bufs = []
    for u in 2 * UNITS:
        h = UT * u
        bufs += [B(2 * h, 128), B(h, 128), B(h, 128), B(UT * NCH, 128), B(2 * h, 128), B(UT, 128)]

    def local_qr(a):
        q1, w2, l1, l2 = pl.pallas_call(
            main_kernel, out_shape=(F(*a.shape), F(N, 256), F(N, N), F(N, N)), in_specs=[V], out_specs=(V,) * 4,
            scratch_shapes=[B(N, N), B(N, 256), B(128, 128), B(128, 128), B(128, 128)] + bufs + [pltpu.SemaphoreType.DMA((2, len(CHUNKS)))] * 8,
            compiler_params=pltpu.CompilerParams(vmem_limit_bytes=34 * 2**20, collective_id=0, has_side_effects=True), name="sweeps")(a)
        return tuple(pl.pallas_call(
            last_kernel, out_shape=(F(*a.shape), F(N, N)), in_specs=[V] * 4, out_specs=(H, H),
            scratch_shapes=[B(*a.shape), B(N, N), pltpu.SemaphoreType.DMA((3,))],
            compiler_params=pltpu.CompilerParams(vmem_limit_bytes=20 * 2**20), name="last")(q1, w2, l2, l1))

    return jax.shard_map(local_qr, mesh=mesh, in_specs=(spec,), out_specs=(spec, P("batch", None)), check_vma=False)
```

```python
import jax
import jax.numpy as jnp
from jax import lax
from jax.experimental import pallas as pl
from jax.experimental.pallas import tpu as pltpu
from jax.sharding import PartitionSpec as P

MESH = pl.DeviceIdType.MESH
HI = lax.Precision.HIGHEST
NN = ((1,), (0,))
TN = ((0,), (0,))
NT = ((1,), (1,))
N = 768
NB = 6
NCH = 64
CHUNKS = ((0, 2, 0), (2, 4, 12), (4, 5, 40), (5, 6, 60))
BLKS = tuple(tuple((i, j) for j in range(a, b) for i in range(j + 1)) for a, b, _ in CHUNKS)
UT = 16
UNITS = tuple(64 * len(b) // UT for b in BLKS)


def dot(a, b, dims):
    return lax.dot_general(a, b, (dims, ((), ())), precision=HI, preferred_element_type=jnp.float32)


def m8(v):
    return pl.multiple_of(v, 8)


def wrap(v):
    return jnp.where(v >= NCH, v - NCH, v)


def rb(i, j=None):
    return slice(128 * i, 128 * (i + 1 if j is None else j))


def bl(x, l):
    return jnp.broadcast_to(x[:, l:l + 1], (8, 128))

def bs(x, s):
    return jnp.broadcast_to(x[s:s + 1, :], (8, 128))

def factor(dref, uref, mref):
    sub = lax.broadcasted_iota(jnp.int32, (8, 128), 0)
    lane = lax.broadcasted_iota(jnp.int32, (8, 128), 1)
    zero = jnp.zeros((8, 128), jnp.float32)
    A = [dref[8 * i:8 * i + 8, :] for i in range(16)]
    for sp in range(8):
        l0 = 16 * sp
        ia, ib = 2 * sp, 2 * sp + 1
        blk = (lane >= l0) & (lane < l0 + 16)
        Ua, Ub = A[ia], A[ib]
        ca = [bl(Ua, l0 + s) for s in range(8)]
        cb = [bl(Ub, l0 + s) for s in range(16)]
        urg = [n for n in (ia + 2, ia + 3) if n < 16]
        cn = {n: [bl(A[n], l0 + s) for s in range(16)] for n in urg}
        Wa = jnp.where(blk, jnp.where(lane == sub + l0, 1.0, zero), Ua)
        Wb = jnp.where(blk, jnp.where(lane == sub + (l0 + 8), 1.0, zero), Ub)
        for n in range(ia + 2, 16):
            A[n] = jnp.where(blk, zero, A[n])
        for s in range(16):
            first = s < 8
            r = s % 8
            ri = lax.rsqrt(bs(ca[s] if first else cb[s], r))
            lb = cb[s] * ri
            if first:
                la = ca[s] * ri
                L = {t: (bs(la, t) if t < 8 else bs(lb, t - 8)) for t in range(s + 1, 16)}
                for t in range(s + 1, 8):
                    ca[t] = ca[t] - la * L[t]
                ma = jnp.where(sub > r, la, zero)
                u, w = bs(Ua, r) * ri, bs(Wa, r) * ri
                Ua = jnp.where(sub == r, u, Ua - ma * u)
                Wa = jnp.where(sub == r, w, Wa - ma * w)
                Ub = Ub - lb * u
                Wb = Wb - lb * w
            else:
                L = {t: bs(lb, t - 8) for t in range(s + 1, 16)}
                mb = jnp.where(sub > r, lb, zero)
                u, w = bs(Ub, r) * ri, bs(Wb, r) * ri
                Ub = jnp.where(sub == r, u, Ub - mb * u)
                Wb = jnp.where(sub == r, w, Wb - mb * w)
            for t in range(s + 1, 16):
                cb[t] = cb[t] - lb * L[t]
            for n in urg:
                ln = cn[n][s] * ri
                for t in range(s + 1, 16):
                    cn[n][t] = cn[n][t] - ln * L[t]
                A[n] = A[n] - ln * w
        uref[l0:l0 + 8, :] = jnp.where(lane >= sub + l0, Ua, zero)
        uref[l0 + 8:l0 + 16, :] = jnp.where(lane >= sub + (l0 + 8), Ub, zero)
        keep = lane < l0 + 16
        mref[l0:l0 + 8, :] = jnp.where(keep, Wa, zero)
        mref[l0 + 8:l0 + 16, :] = jnp.where(keep, Wb, zero)
        if ia + 4 < 16:
            W = jnp.concatenate([Wa, Wb], axis=0)
            D = dot(W, W, ((0,), (0,)))
            for n in range(ia + 4, 16):
                A[n] = A[n] - D[8 * n:8 * n + 8, :]


class Sum:
    def __init__(self, ch, c, me, bufs, sems):
        self.ch, self.c, self.me, self.other = ch, c, me, 1 - c
        self.p, self.recv0, self.acc, self.recv1, self.o, self.red = bufs
        self.s0, self.r0, self.s1, self.r1, self.s2, self.r2, self.s3, self.r3 = sems
        self.U = UNITS[ch]
        self.half = UT * self.U
        self.base = wrap(CHUNKS[ch][2] + 32 * c)
        self.mine = pl.ds(m8(c * self.half), self.half)
        self.unit = lax.rem(13 * (me - self.base + NCH), NCH)

    def gram(self, x):
        a, b, _ = CHUNKS[self.ch]
        if b - a == 2:
            full = dot(x[:, rb(0, b)], x[:, rb(a, b)], TN)
        else:
            full = dot(x[:, rb(a, b)], x[:, rb(0, b)], TN)
        for n, (i, j) in enumerate(BLKS[self.ch]):
            self.p[rb(n), :] = full[rb(i), rb(j - a)] if b - a == 2 else full[:, rb(i)].T

    def exch(self, ref, dst, s, r, sl):
        return pltpu.make_async_remote_copy(ref.at[sl], dst, s, r, device_id=(0, self.other, self.me), device_id_type=MESH)

    def swap(self):
        sl = pl.ds(m8(self.other * self.half), self.half)
        self.cp0 = self.exch(self.p, self.recv0, self.s0, self.r0, sl)
        self.cp0.start()

    def scatter(self):
        self.exch(self.p, self.recv0, self.s0, self.r0, self.mine).wait_recv()
        self.acc[...] = self.p[self.mine] + self.recv0[...]
        slot = pl.ds(m8(UT * self.me), UT)
        first = lax.rem(self.me, self.U)

        def send(i, _):
            u = first + i
            u = jnp.where(u >= self.U, u - self.U, u)
            peer = lax.rem(self.base + 5 * u, NCH)

            @pl.when(peer != self.me)
            def _():
                pltpu.make_async_remote_copy(self.acc.at[pl.ds(m8(UT * u), UT)], self.recv1.at[slot], self.s1, self.r1, device_id=(0, self.c, peer), device_id_type=MESH).start()
            return 0
        lax.fori_loop(0, self.U, send, 0, unroll=4)

    def rows(self, n, s, r):
        return pltpu.make_async_remote_copy(self.recv1.at[pl.ds(0, UT * n)], self.recv1.at[pl.ds(0, UT * n)], s, r, device_id=(0, self.other, self.me), device_id_type=MESH)

    def reduce(self):
        @pl.when(self.unit < self.U)
        def _():
            self.recv1[pl.ds(m8(UT * self.me), UT)] = self.acc[pl.ds(m8(UT * self.unit), UT)]
            self.rows(63, self.s1, self.r1).wait_recv()
            t = [self.recv1[UT * k:UT * k + UT, :] for k in range(NCH)]
            while len(t) > 1:
                t = [t[i] + t[i + 1] for i in range(0, len(t), 2)]
            self.red[...] = t[0]
            dst = pl.ds(m8(self.c * self.half + UT * self.unit), UT)

            def send(k, _):
                pltpu.make_async_remote_copy(self.red, self.o.at[dst], self.s2, self.r2, device_id=(0, self.c, wrap(self.me + k)), device_id_type=MESH).start()
                return 0
            lax.fori_loop(1, NCH, send, 0, unroll=7)
            self.o[dst] = t[0]

    def gather(self):
        @pl.when(self.unit < self.U)
        def _():
            self.rows(self.U - 1, self.s2, self.r2).wait_recv()

        @pl.when(self.unit >= self.U)
        def _():
            self.rows(self.U, self.s2, self.r2).wait_recv()
        self.exch(self.o, self.o.at[self.mine], self.s3, self.r3, self.mine).start()

    def finish(self, g):
        self.exch(self.o, self.o.at[self.mine], self.s3, self.r3, self.mine).wait_recv()
        for n, (i, j) in enumerate(BLKS[self.ch]):
            g[rb(i), rb(j)] = self.o[rb(n), :]

    def drain(self):
        self.exch(self.p, self.recv0, self.s0, self.r0, self.mine).wait_send()
        self.exch(self.o, self.o.at[self.mine], self.s3, self.r3, self.mine).wait_send()

        @pl.when(self.unit < self.U)
        def _():
            self.rows(self.U - 1, self.s1, self.r1).wait_send()
            self.rows(63, self.s2, self.r2).wait_send()

        @pl.when(self.unit >= self.U)
        def _():
            self.rows(self.U, self.s1, self.r1).wait_send()


def greet(c, me):
    bar = pltpu.get_barrier_semaphore()
    pl.semaphore_signal(bar, inc=1, device_id=(0, 1 - c, me), device_id_type=MESH)

    def sig(k, _):
        pl.semaphore_signal(bar, inc=1, device_id=(0, c, wrap(me + k)), device_id_type=MESH)
        return 0
    lax.fori_loop(1, NCH, sig, 0, unroll=7)
    return bar


def eliminate(j, a, b, g, u, w):
    if a < b:
        v = dot(w[rb(j), :], g[rb(j), rb(a, b)], NN)
        u[rb(j), rb(a, b)] = v
        for m in range(j + 1, b, 2):
            lo, hi = max(a, m), min(m + 2, b)
            g[rb(m, hi), rb(lo, b)] = g[rb(m, hi), rb(lo, b)] - dot(u[rb(j), rb(m, hi)], v[:, 128 * (lo - a):], TN)


def invert_pair(k, u, w, wt):
    t = w[rb(k), :].T
    wt[rb(k), rb(k % 2)] = t
    if k % 2:
        wt[rb(k - 1), rb(1)] = -dot(wt[rb(k - 1), rb(0)], dot(u[rb(k - 1), rb(k)], t, NN), NN)


def solve_rows(x_ref, u, wt, q_ref, a, b, sl):
    t = x_ref[sl, rb(a, b)]
    if a:
        t = t - dot(q_ref[sl, rb(0, a)], u[rb(0, a), rb(a, b)], NN)
    q_ref[sl, rb(a, b)] = dot(t, wt[rb(a, b), :] if b - a == 2 else wt[rb(a), rb(a % 2)], NN)


def solve_cols(x_ref, u, wt, q_ref, a, b):
    def rows(r, _):
        solve_rows(x_ref, u, wt, q_ref, a, b, pl.ds(pl.multiple_of(256 * r, 256), 256))
        return 0
    lax.fori_loop(0, x_ref.shape[0] // 256, rows, 0)


JOIN = ((-1, 1, 2, 2), (5, 7, 8, 10))
GATHER = ((-1, 0, 1, 1), (4, 6, 8, 10))
REDUCE = ((-1, -1, -1, 0), (3, 5, 6, 8))
SCATTER = ((-1, -1, -1, -1), (2, 4, 5, 6))
APPLY = {1: 0, 3: 1, 4: 2, 5: 3}


def main_kernel(xin, q, wt2, u1, u2, x, xsem, g, wt1, w, dbuf, ubuf, mbuf, *rest):
    c, me = lax.axis_index("outer"), lax.axis_index("rows")
    load = [pltpu.make_async_copy(xin.at[:, rb(2 * j, 2 * j + 2)], x.at[:, rb(2 * j, 2 * j + 2)], xsem.at[j]) for j in range(3)]
    for cp in load:
        cp.start()
    bar = greet(c, me)
    nc = len(CHUNKS)
    bufs, sems = rest[:12 * nc], rest[12 * nc:]
    S = [[Sum(ch, c, me, bufs[6 * (nc * s + ch):6 * (nc * s + ch) + 6], [r.at[s, ch] for r in sems]) for ch in range(nc)] for s in range(2)]
    S0, S1 = S
    for r in (wt1, wt2, u1, u2):
        r[...] = jnp.zeros_like(r)
    for ch in range(2):
        load[ch].wait()
        S0[ch].gram(x)
    load[2].wait()
    pl.semaphore_wait(bar, NCH)
    for ch in range(2):
        S0[ch].swap()
    S0[2].gram(x)
    S0[2].swap()
    for ch in range(2):
        S0[ch].scatter()
    S0[3].gram(x)
    S0[3].swap()
    for ch in (2, 3):
        S0[ch].scatter()
    for ch in range(3):
        S0[ch].reduce()
    S0[0].gather()
    S0[0].finish(g)
    dbuf[...] = g[rb(0), rb(0)]

    def section(t):
        s, k = divmod(t, NB)
        u, wt = ((u1, wt1), (u2, wt2))[s]
        for ss in range(2):
            for ch in range(nc):
                if SCATTER[ss][ch] == t:
                    S[ss][ch].scatter()
        for ss in range(2):
            for ch in range(nc):
                if REDUCE[ss][ch] == t:
                    S[ss][ch].reduce()
        for ss in range(2):
            for ch in range(nc):
                if GATHER[ss][ch] == t:
                    S[ss][ch].gather()
        w[rb(k), :] = mbuf[...]
        u[rb(k), rb(k)] = ubuf[...]
        end = max(CHUNKS[ch][1] for ch in range(nc) if JOIN[s][ch] < t)
        eliminate(k, k + 1, end, g, u, w)
        for ch in range(nc):
            if JOIN[s][ch] == t:
                S[s][ch].finish(g)
                a, b, _ = CHUNKS[ch]
                for j in range(k + 1):
                    eliminate(j, a, b, g, u, w)
        if k < NB - 1:
            dbuf[...] = g[rb(k + 1), rb(k + 1)]
        invert_pair(k, u, w, wt)
        if t in APPLY:
            ch = APPLY[t]
            a, b, _ = CHUNKS[ch]
            solve_cols(x, u, wt, q, a, b)
            S1[ch].gram(q)
            S1[ch].swap()
        if t == NB - 1:
            S1[0].finish(g)
            dbuf[...] = g[rb(0), rb(0)]

    def step(t, _):
        factor(dbuf, ubuf, mbuf)
        for tt in range(2 * NB):
            @pl.when(t == tt)
            def _():
                section(tt)
        return 0

    lax.fori_loop(0, 2 * NB, step, 0)
    for s in S:
        for ch in s:
            ch.drain()


def last_kernel(x, wt, u2, u1, qo, ro, q, r, sem):
    def blk(i):
        return pl.ds(pl.multiple_of(256 * i, 256), 256)

    for i in range(3):
        for j in range(i):
            r[rb(2 * i, 2 * i + 2), rb(2 * j, 2 * j + 2)] = jnp.zeros((256, 256), jnp.float32)

    def diag(d):
        def f(i, _):
            k = pl.ds(pl.multiple_of(256 * i, 256), 256 * (d + 1))
            r[blk(i), blk(i + d)] = dot(u2[blk(i), k], u1[k, blk(i + d)], NN)
            return 0
        lax.fori_loop(0, 3 - d, f, 0)
    for d in range(3):
        diag(d)
    out = pltpu.make_async_copy(r, ro, sem.at[0])
    out.start()
    part = x.shape[0] // 4

    def rows(h, _):
        sl = pl.ds(pl.multiple_of(part * h, part), part)
        for j in range(3):
            solve_rows(x, u2, wt, q, 2 * j, 2 * j + 2, sl)
        pltpu.make_async_copy(q.at[sl], qo.at[sl], sem.at[h + 1]).start()
        return 0
    lax.fori_loop(0, 4, rows, 0)
    for h in range(4):
        sl = pl.ds(part * h, part)
        pltpu.make_async_copy(q.at[sl], qo.at[sl], sem.at[h + 1]).wait()
    out.wait()


def solution(mesh):
    spec = P(("batch", "outer", "rows"), None)
    V = pl.BlockSpec(memory_space=pltpu.VMEM)
    H = pl.BlockSpec(memory_space=pl.ANY)
    F = lambda *s: jax.ShapeDtypeStruct(s, jnp.float32)
    B = lambda *s: pltpu.VMEM(s, jnp.float32)
    bufs = []
    for u in 2 * UNITS:
        h = UT * u
        bufs += [B(2 * h, 128), B(h, 128), B(h, 128), B(UT * NCH, 128), B(2 * h, 128), B(UT, 128)]

    def local_qr(a):
        q1, wt2, u1, u2 = pl.pallas_call(
            main_kernel, out_shape=(F(*a.shape), F(N, 256), F(N, N), F(N, N)), in_specs=[pl.BlockSpec(memory_space=pltpu.HBM)], out_specs=(V,) * 4,
            scratch_shapes=[B(*a.shape), pltpu.SemaphoreType.DMA((3,)), B(N, N), B(N, 256), B(N, 128), B(128, 128), B(128, 128), B(128, 128)] + bufs + [pltpu.SemaphoreType.DMA((2, len(CHUNKS)))] * 8,
            compiler_params=pltpu.CompilerParams(vmem_limit_bytes=44 * 2**20, collective_id=0, has_side_effects=True), name="sweeps")(a)
        return tuple(pl.pallas_call(
            last_kernel, out_shape=(F(*a.shape), F(N, N)), in_specs=[V] * 4, out_specs=(H, H),
            scratch_shapes=[B(*a.shape), B(N, N), pltpu.SemaphoreType.DMA((5,))],
            compiler_params=pltpu.CompilerParams(vmem_limit_bytes=20 * 2**20), name="last")(q1, wt2, u2, u1))

    return jax.shard_map(local_qr, mesh=mesh, in_specs=(spec,), out_specs=(spec, P("batch", None)), check_vma=False)
```

```python
import jax
import jax.numpy as jnp
from jax import lax
from jax.experimental import pallas as pl
from jax.experimental.pallas import tpu as pltpu
from jax.sharding import PartitionSpec as P

MESH = pl.DeviceIdType.MESH
HI = lax.Precision.HIGHEST
NN = ((1,), (0,))
TN = ((0,), (0,))
NT = ((1,), (1,))
N = 768
NB = 6
NCH = 64
CHUNKS = ((0, 2, 0), (2, 4, 12), (4, 5, 40), (5, 6, 60))
BLKS = tuple(tuple((i, j) for j in range(a, b) for i in range(j + 1)) for a, b, _ in CHUNKS)
UT = 16
UNITS = tuple(64 * len(b) // UT for b in BLKS)


def dot(a, b, dims):
    return lax.dot_general(a, b, (dims, ((), ())), precision=HI, preferred_element_type=jnp.float32)


def m8(v):
    return pl.multiple_of(v, 8)


def wrap(v):
    return jnp.where(v >= NCH, v - NCH, v)


def rb(i, j=None):
    return slice(128 * i, 128 * (i + 1 if j is None else j))


def bl(x, l):
    return jnp.broadcast_to(x[:, l:l + 1], (8, 128))

def bs(x, s):
    return jnp.broadcast_to(x[s:s + 1, :], (8, 128))

def factor(dref, uref, mref):
    sub = lax.broadcasted_iota(jnp.int32, (8, 128), 0)
    lane = lax.broadcasted_iota(jnp.int32, (8, 128), 1)
    zero = jnp.zeros((8, 128), jnp.float32)
    A = [dref[8 * i:8 * i + 8, :] for i in range(16)]
    for sp in range(8):
        l0 = 16 * sp
        ia, ib = 2 * sp, 2 * sp + 1
        blk = (lane >= l0) & (lane < l0 + 16)
        Ua, Ub = A[ia], A[ib]
        ca = [bl(Ua, l0 + s) for s in range(8)]
        cb = [bl(Ub, l0 + s) for s in range(16)]
        urg = [n for n in (ia + 2, ia + 3) if n < 16]
        cn = {n: [bl(A[n], l0 + s) for s in range(16)] for n in urg}
        Wa = jnp.where(blk, jnp.where(lane == sub + l0, 1.0, zero), Ua)
        Wb = jnp.where(blk, jnp.where(lane == sub + (l0 + 8), 1.0, zero), Ub)
        for n in range(ia + 2, 16):
            A[n] = jnp.where(blk, zero, A[n])
        for s in range(16):
            first = s < 8
            r = s % 8
            ri = lax.rsqrt(bs(ca[s] if first else cb[s], r))
            lb = cb[s] * ri
            if first:
                la = ca[s] * ri
                L = {t: (bs(la, t) if t < 8 else bs(lb, t - 8)) for t in range(s + 1, 16)}
                for t in range(s + 1, 8):
                    ca[t] = ca[t] - la * L[t]
                ma = jnp.where(sub > r, la, zero)
                u, w = bs(Ua, r) * ri, bs(Wa, r) * ri
                Ua = jnp.where(sub == r, u, Ua - ma * u)
                Wa = jnp.where(sub == r, w, Wa - ma * w)
                Ub = Ub - lb * u
                Wb = Wb - lb * w
            else:
                L = {t: bs(lb, t - 8) for t in range(s + 1, 16)}
                mb = jnp.where(sub > r, lb, zero)
                u, w = bs(Ub, r) * ri, bs(Wb, r) * ri
                Ub = jnp.where(sub == r, u, Ub - mb * u)
                Wb = jnp.where(sub == r, w, Wb - mb * w)
            for t in range(s + 1, 16):
                cb[t] = cb[t] - lb * L[t]
            for n in urg:
                ln = cn[n][s] * ri
                for t in range(s + 1, 16):
                    cn[n][t] = cn[n][t] - ln * L[t]
                A[n] = A[n] - ln * w
        uref[l0:l0 + 8, :] = jnp.where(lane >= sub + l0, Ua, zero)
        uref[l0 + 8:l0 + 16, :] = jnp.where(lane >= sub + (l0 + 8), Ub, zero)
        keep = lane < l0 + 16
        mref[l0:l0 + 8, :] = jnp.where(keep, Wa, zero)
        mref[l0 + 8:l0 + 16, :] = jnp.where(keep, Wb, zero)
        if ia + 4 < 16:
            W = jnp.concatenate([Wa, Wb], axis=0)
            D = dot(W, W, ((0,), (0,)))
            for n in range(ia + 4, 16):
                A[n] = A[n] - D[8 * n:8 * n + 8, :]


class Sum:
    def __init__(self, ch, c, me, bufs, sems):
        self.ch, self.c, self.me, self.other = ch, c, me, 1 - c
        self.p, self.recv0, self.acc, self.recv1, self.o, self.red = bufs
        self.s0, self.r0, self.s1, self.r1, self.s2, self.r2, self.s3, self.r3 = sems
        self.U = UNITS[ch]
        self.half = UT * self.U
        self.base = wrap(CHUNKS[ch][2] + 32 * c)
        self.mine = pl.ds(m8(c * self.half), self.half)
        self.unit = lax.rem(13 * (me - self.base + NCH), NCH)

    def gram(self, x):
        a, b, _ = CHUNKS[self.ch]
        if b - a == 2:
            full = dot(x[:, rb(0, b)], x[:, rb(a, b)], TN)
        else:
            full = dot(x[:, rb(a, b)], x[:, rb(0, b)], TN)
        for n, (i, j) in enumerate(BLKS[self.ch]):
            self.p[rb(n), :] = full[rb(i), rb(j - a)] if b - a == 2 else full[:, rb(i)].T

    def exch(self, ref, dst, s, r, sl):
        return pltpu.make_async_remote_copy(ref.at[sl], dst, s, r, device_id=(0, self.other, self.me), device_id_type=MESH)

    def swap(self):
        sl = pl.ds(m8(self.other * self.half), self.half)
        self.cp0 = self.exch(self.p, self.recv0, self.s0, self.r0, sl)
        self.cp0.start()

    def scatter(self):
        self.exch(self.p, self.recv0, self.s0, self.r0, self.mine).wait_recv()
        self.acc[...] = self.p[self.mine] + self.recv0[...]
        slot = pl.ds(m8(UT * self.me), UT)
        first = lax.rem(self.me, self.U)

        def send(i, _):
            u = first + i
            u = jnp.where(u >= self.U, u - self.U, u)
            peer = lax.rem(self.base + 5 * u, NCH)

            @pl.when(peer != self.me)
            def _():
                pltpu.make_async_remote_copy(self.acc.at[pl.ds(m8(UT * u), UT)], self.recv1.at[slot], self.s1, self.r1, device_id=(0, self.c, peer), device_id_type=MESH).start()
            return 0
        lax.fori_loop(0, self.U, send, 0, unroll=4)

    def rows(self, n, s, r):
        return pltpu.make_async_remote_copy(self.recv1.at[pl.ds(0, UT * n)], self.recv1.at[pl.ds(0, UT * n)], s, r, device_id=(0, self.other, self.me), device_id_type=MESH)

    def reduce(self):
        @pl.when(self.unit < self.U)
        def _():
            self.recv1[pl.ds(m8(UT * self.me), UT)] = self.acc[pl.ds(m8(UT * self.unit), UT)]
            self.rows(63, self.s1, self.r1).wait_recv()
            t = [self.recv1[UT * k:UT * k + UT, :] for k in range(NCH)]
            while len(t) > 1:
                t = [t[i] + t[i + 1] for i in range(0, len(t), 2)]
            self.red[...] = t[0]
            dst = pl.ds(m8(self.c * self.half + UT * self.unit), UT)

            def send(k, _):
                pltpu.make_async_remote_copy(self.red, self.o.at[dst], self.s2, self.r2, device_id=(0, self.c, wrap(self.me + k)), device_id_type=MESH).start()
                return 0
            lax.fori_loop(1, NCH, send, 0, unroll=7)
            self.o[dst] = t[0]

    def gather(self):
        @pl.when(self.unit < self.U)
        def _():
            self.rows(self.U - 1, self.s2, self.r2).wait_recv()

        @pl.when(self.unit >= self.U)
        def _():
            self.rows(self.U, self.s2, self.r2).wait_recv()
        self.exch(self.o, self.o.at[self.mine], self.s3, self.r3, self.mine).start()

    def finish(self, g):
        self.exch(self.o, self.o.at[self.mine], self.s3, self.r3, self.mine).wait_recv()
        for n, (i, j) in enumerate(BLKS[self.ch]):
            g[rb(i), rb(j)] = self.o[rb(n), :]

    def drain(self):
        self.exch(self.p, self.recv0, self.s0, self.r0, self.mine).wait_send()
        self.exch(self.o, self.o.at[self.mine], self.s3, self.r3, self.mine).wait_send()

        @pl.when(self.unit < self.U)
        def _():
            self.rows(self.U - 1, self.s1, self.r1).wait_send()
            self.rows(63, self.s2, self.r2).wait_send()

        @pl.when(self.unit >= self.U)
        def _():
            self.rows(self.U, self.s1, self.r1).wait_send()


def greet(c, me):
    bar = pltpu.get_barrier_semaphore()
    pl.semaphore_signal(bar, inc=1, device_id=(0, 1 - c, me), device_id_type=MESH)

    def sig(k, _):
        pl.semaphore_signal(bar, inc=1, device_id=(0, c, wrap(me + k)), device_id_type=MESH)
        return 0
    lax.fori_loop(1, NCH, sig, 0, unroll=7)
    return bar


def eliminate(j, a, b, g, u, w):
    if a < b:
        v = dot(w[rb(j), :], g[rb(j), rb(a, b)], NN)
        u[rb(j), rb(a, b)] = v
        for m in range(j + 1, b, 2):
            lo, hi = max(a, m), min(m + 2, b)
            g[rb(m, hi), rb(lo, b)] = g[rb(m, hi), rb(lo, b)] - dot(u[rb(j), rb(m, hi)], v[:, 128 * (lo - a):], TN)


def invert_pair(k, u, w, wt):
    t = w[rb(k), :].T
    wt[rb(k), rb(k % 2)] = t
    if k % 2:
        wt[rb(k - 1), rb(1)] = -dot(wt[rb(k - 1), rb(0)], dot(u[rb(k - 1), rb(k)], t, NN), NN)


def solve_rows(x_ref, u, wt, q_ref, a, b, sl):
    t = x_ref[sl, rb(a, b)]
    if a:
        t = t - dot(q_ref[sl, rb(0, a)], u[rb(0, a), rb(a, b)], NN)
    q_ref[sl, rb(a, b)] = dot(t, wt[rb(a, b), :] if b - a == 2 else wt[rb(a), rb(a % 2)], NN)


def solve_cols(x_ref, u, wt, q_ref, a, b):
    def rows(r, _):
        solve_rows(x_ref, u, wt, q_ref, a, b, pl.ds(pl.multiple_of(256 * r, 256), 256))
        return 0
    lax.fori_loop(0, x_ref.shape[0] // 256, rows, 0)


JOIN = ((-1, 1, 2, 2), (5, 7, 8, 10))
GATHER = ((-1, 0, 1, 1), (4, 6, 8, 10))
REDUCE = ((-1, -1, -1, 0), (3, 5, 6, 8))
SCATTER = ((-1, -1, -1, -1), (2, 4, 5, 6))
APPLY = {1: 0, 3: 1, 4: 2, 5: 3}


def main_kernel(xin, q, wt2, u1, u2, x, xsem, g, wt1, w, dbuf, ubuf, mbuf, *rest):
    c, me = lax.axis_index("outer"), lax.axis_index("rows")
    load = [pltpu.make_async_copy(xin.at[:, rb(2 * j, 2 * j + 2)], x.at[:, rb(2 * j, 2 * j + 2)], xsem.at[j]) for j in range(3)]
    for cp in load:
        cp.start()
    bar = greet(c, me)
    nc = len(CHUNKS)
    bufs, sems = rest[:12 * nc], rest[12 * nc:]
    S = [[Sum(ch, c, me, bufs[6 * (nc * s + ch):6 * (nc * s + ch) + 6], [r.at[s, ch] for r in sems]) for ch in range(nc)] for s in range(2)]
    S0, S1 = S
    for k in range(1, NB, 2):
        for r, j in ((u1, k - 1), (u2, k - 1), (wt1, 0), (wt2, 0)):
            r[rb(k), rb(j)] = jnp.zeros((128, 128), jnp.float32)
    for ch in range(2):
        load[ch].wait()
        S0[ch].gram(x)
    load[2].wait()
    pl.semaphore_wait(bar, NCH)
    for ch in range(2):
        S0[ch].swap()
    S0[2].gram(x)
    S0[2].swap()
    for ch in range(2):
        S0[ch].scatter()
    S0[3].gram(x)
    S0[3].swap()
    S0[2].scatter()
    S0[0].reduce()
    S0[3].scatter()
    for ch in (1, 2):
        S0[ch].reduce()
    S0[0].gather()
    S0[0].finish(g)
    dbuf[...] = g[rb(0), rb(0)]

    def section(t):
        s, k = divmod(t, NB)
        u, wt = ((u1, wt1), (u2, wt2))[s]
        for ss in range(2):
            for ch in range(nc):
                if SCATTER[ss][ch] == t:
                    S[ss][ch].scatter()
        for ss in range(2):
            for ch in range(nc):
                if REDUCE[ss][ch] == t:
                    S[ss][ch].reduce()
        for ss in range(2):
            for ch in range(nc):
                if GATHER[ss][ch] == t:
                    S[ss][ch].gather()
        w[rb(k), :] = mbuf[...]
        u[rb(k), rb(k)] = ubuf[...]
        end = max(CHUNKS[ch][1] for ch in range(nc) if JOIN[s][ch] < t)
        eliminate(k, k + 1, end, g, u, w)
        for ch in range(nc):
            if JOIN[s][ch] == t:
                S[s][ch].finish(g)
                a, b, _ = CHUNKS[ch]
                for j in range(k + 1):
                    eliminate(j, a, b, g, u, w)
        if k < NB - 1:
            dbuf[...] = g[rb(k + 1), rb(k + 1)]
        invert_pair(k, u, w, wt)
        if t in APPLY:
            ch = APPLY[t]
            a, b, _ = CHUNKS[ch]
            solve_cols(x, u, wt, q, a, b)
            S1[ch].gram(q)
            S1[ch].swap()
        if t == NB - 1:
            S1[0].finish(g)
            dbuf[...] = g[rb(0), rb(0)]

    def step(t, _):
        factor(dbuf, ubuf, mbuf)
        for tt in range(2 * NB):
            @pl.when(t == tt)
            def _():
                section(tt)
        return 0

    lax.fori_loop(0, 2 * NB, step, 0)
    for s in S:
        for ch in s:
            ch.drain()


def last_kernel(x, wt, u2, u1, qo, ro, q, r, sem):
    def blk(i):
        return pl.ds(pl.multiple_of(256 * i, 256), 256)

    for i in range(3):
        for j in range(i):
            r[rb(2 * i, 2 * i + 2), rb(2 * j, 2 * j + 2)] = jnp.zeros((256, 256), jnp.float32)

    def diag(d):
        def f(i, _):
            k = pl.ds(pl.multiple_of(256 * i, 256), 256 * (d + 1))
            r[blk(i), blk(i + d)] = dot(u2[blk(i), k], u1[k, blk(i + d)], NN)
            return 0
        lax.fori_loop(0, 3 - d, f, 0)
    for d in range(3):
        diag(d)
    out = pltpu.make_async_copy(r, ro, sem.at[0])
    out.start()
    part = x.shape[0] // 4

    def rows(h, _):
        sl = pl.ds(pl.multiple_of(part * h, part), part)
        for j in range(3):
            solve_rows(x, u2, wt, q, 2 * j, 2 * j + 2, sl)
        pltpu.make_async_copy(q.at[sl], qo.at[sl], sem.at[h + 1]).start()
        return 0
    lax.fori_loop(0, 4, rows, 0)
    for h in range(4):
        sl = pl.ds(part * h, part)
        pltpu.make_async_copy(q.at[sl], qo.at[sl], sem.at[h + 1]).wait()
    out.wait()


def solution(mesh):
    spec = P(("batch", "outer", "rows"), None)
    V = pl.BlockSpec(memory_space=pltpu.VMEM)
    H = pl.BlockSpec(memory_space=pl.ANY)
    F = lambda *s: jax.ShapeDtypeStruct(s, jnp.float32)
    B = lambda *s: pltpu.VMEM(s, jnp.float32)
    bufs = []
    for u in 2 * UNITS:
        h = UT * u
        bufs += [B(2 * h, 128), B(h, 128), B(h, 128), B(UT * NCH, 128), B(2 * h, 128), B(UT, 128)]

    def local_qr(a):
        q1, wt2, u1, u2 = pl.pallas_call(
            main_kernel, out_shape=(F(*a.shape), F(N, 256), F(N, N), F(N, N)), in_specs=[pl.BlockSpec(memory_space=pltpu.HBM)], out_specs=(V,) * 4,
            scratch_shapes=[B(*a.shape), pltpu.SemaphoreType.DMA((3,)), B(N, N), B(N, 256), B(N, 128), B(128, 128), B(128, 128), B(128, 128)] + bufs + [pltpu.SemaphoreType.DMA((2, len(CHUNKS)))] * 8,
            compiler_params=pltpu.CompilerParams(vmem_limit_bytes=44 * 2**20, collective_id=0, has_side_effects=True), name="sweeps")(a)
        return tuple(pl.pallas_call(
            last_kernel, out_shape=(F(*a.shape), F(N, N)), in_specs=[V] * 4, out_specs=(H, H),
            scratch_shapes=[B(*a.shape), B(N, N), pltpu.SemaphoreType.DMA((5,))],
            compiler_params=pltpu.CompilerParams(vmem_limit_bytes=20 * 2**20), name="last")(q1, wt2, u2, u1))

    return jax.shard_map(local_qr, mesh=mesh, in_specs=(spec,), out_specs=(spec, P("batch", None)), check_vma=False)
```
